32 devices in a mesh: dp: 4 (over y, x), cls: 8 (over z, core).
Axes of the slice: x: 2, y: 2, z: 4, core: 2. Of those that a mesh axis runs over, the one named last changes fastest.
Arguments:
- sketches: bfloat16 [8192, 4096], P(('dp', 'cls')), may hold values from -6 to 6
- labels: int32 [8192], P(('dp', 'cls')), may hold values from 0 to 7, as said below
- places: int32 [8192], P(('dp', 'cls')), may hold values from 0 to 2047, as said below
- counts: int32 [8, 4, 32], P('cls'), may hold values from 0 to 16, as said below
- chosen: int32 [3, 8], P(None, 'cls'), may hold values from 0 to 2047, as said below
Outputs:
- gain_scores: float32 [3, 8, 2048], P(None, 'cls', 'dp')
- coverage: float32 [8, 2048], P('cls', 'dp')
The draws below stay inside these ranges and needn't reach their ends.
Inputs may be any that keep to these rules, and one draw needn't show every extreme that they name: `labels`: every class has 4 or more examples. `places`: an example of device s (its index along dp and cls together) with class k has place m * 512 + s * 16 + j in class k's block: m is the member of dp that receives it, and for each k, m and s the j run over 0 to counts[k, m, s] - 1 without gaps, so no two examples share a place. In every draw one class and member receive 16 examples from every device. counts[k, m, s] is the number of examples of device s that take places of class k on member m. chosen[t, k] is a place of class k's block that holds an example; the 3 picks of a class differ.
All inputs are finite; a program needn't handle non-finite values.
Results may differ from the reference program's by a relative error of at most 0.0003.
Values may be sent and summed in bfloat16 or wider, within the bound.
A program may use at most 128 MiB of HBM per device.

```python
import jax
import jax.numpy as jnp
from jax import lax

D = 4096
ROW_DEV = 256
STEPS = 3
CLASSES = 8
SUB = 16
CAP = 512
BLOCK = 2048
ROWS = 8192
N_DP = 4
DEVICES = 32


def layout_tables(key):
    slot_count = 2 * ROW_DEV
    class_key, full_key, member_key, base_key, pick_key = jax.random.split(jax.random.fold_in(key, 7), 5)
    class_level = jax.random.randint(class_key, (CLASSES,), 0, 3)
    full_class = jax.random.randint(full_key, (), 0, CLASSES)
    full_member = jax.random.randint(member_key, (), 0, N_DP)
    item_index = jnp.arange(slot_count, dtype=jnp.int32)
    item_member = item_index // (CLASSES * SUB)
    item_class = item_index // SUB % CLASSES
    item_place = item_index % SUB
    source = jnp.arange(DEVICES, dtype=jnp.int32)[:, None]
    promised = (item_class[None, :] == source % CLASSES) & (item_member[None, :] == source // CLASSES % N_DP) & (item_place[None, :] == 0)
    full_item = (item_class == full_class) & (item_member == full_member)
    base = jax.random.randint(base_key, (DEVICES, slot_count), 0, 2 ** 16)
    level = base + class_level[item_class][None, :] * 2 ** 16 + promised.astype(jnp.int32) * 2 ** 18 + full_item.astype(jnp.int32)[None, :] * 2 ** 19
    score = level * slot_count + item_index[None, :]
    top_scores, picked_items = lax.top_k(score, ROW_DEV)
    group = picked_items // SUB
    same_group = group[:, :, None] == group[:, None, :]
    earlier = picked_items[:, None, :] < picked_items[:, :, None]
    rank = jnp.sum((same_group & earlier).astype(jnp.int32), axis=2)
    member = group // CLASSES
    klass = group % CLASSES
    places = member * CAP + source * SUB + rank
    group_hits = (group[:, :, None] == jnp.arange(N_DP * CLASSES, dtype=jnp.int32)[None, None, :]).astype(jnp.int32)
    per_group = jnp.sum(group_hits, axis=1).reshape(DEVICES, N_DP, CLASSES)
    counts = jnp.transpose(per_group, (2, 1, 0))
    valid = (jnp.arange(SUB, dtype=jnp.int32)[None, None, None, :] < counts[:, :, :, None]).reshape(CLASSES, BLOCK)
    noise = jax.random.randint(pick_key, (CLASSES, BLOCK), 0, 256)
    pick_score = (noise + valid.astype(jnp.int32) * 512) * BLOCK + jnp.arange(BLOCK, dtype=jnp.int32)[None, :]
    top_picks, pick_places = lax.top_k(pick_score, STEPS)
    return (klass.reshape(-1), places.reshape(-1), counts, jnp.transpose(pick_places))


def draw_labels(key, part):
    return layout_tables(key)[0].astype(jnp.int32)


def draw_places(key, part):
    return layout_tables(key)[1].astype(jnp.int32)


def draw_counts(key, part):
    return layout_tables(key)[2].astype(jnp.int32)


def draw_chosen(key, part):
    return layout_tables(key)[3].astype(jnp.int32)


def draw_sketches(key, part):
    labels = layout_tables(key)[0].astype(jnp.int32)
    mean_key, noise_key, scale_key = jax.random.split(jax.random.fold_in(key, 11), 3)
    class_means = jnp.clip(jax.random.normal(mean_key, (CLASSES, D), jnp.float32), -4.2, 4.2)
    centers = 0.6 * class_means[labels]
    noise = jnp.clip(jax.random.normal(noise_key, (ROWS, D), jnp.float32), -4.2, 4.2)
    raw = centers + noise
    row_rms = jnp.sqrt(jnp.mean(raw * raw, axis=1, keepdims=True))
    scale = jnp.exp(jax.random.uniform(scale_key, (ROWS, 1), jnp.float32, jnp.log(0.98), jnp.log(1.02)))
    values = jnp.clip(scale * raw / row_rms, -6.0, 6.0)
    return values.astype(jnp.bfloat16)


def setup_inputs(seed: int = 0) -> dict:
    seeds = jax.random.split(jax.random.key(seed), 6)
    sketches = draw_sketches(jax.random.fold_in(seeds[5], 71), 0)
    labels = draw_labels(jax.random.fold_in(seeds[5], 71), 0)
    places = draw_places(jax.random.fold_in(seeds[5], 71), 0)
    counts = draw_counts(jax.random.fold_in(seeds[5], 71), 0)
    chosen = draw_chosen(jax.random.fold_in(seeds[5], 71), 0)
    return {"sketches": sketches, "labels": labels, "places": places, "counts": counts, "chosen": chosen}


def class_scores(class_block, class_counts, class_picks):
    wide = class_block.astype(jnp.float32)
    norms = jnp.sum(wide * wide, axis=1)
    inner = jnp.dot(class_block, class_block.T, preferred_element_type=jnp.float32)
    spread = (norms[:, None] + norms[None, :] - 2.0 * inner) / D
    valid = (jnp.arange(SUB, dtype=jnp.int32)[None, None, :] < class_counts[:, :, None]).reshape(-1)
    weight = valid.astype(jnp.float32)
    bound = jnp.max(jnp.where(valid[:, None] & valid[None, :], spread, 0.0))
    similar = bound - spread
    total = jnp.sum(class_counts).astype(jnp.float32)
    cover = jnp.zeros((similar.shape[0],), jnp.float32)
    scores = []
    for turn_index in range(STEPS):
        scores.append(jnp.sum(weight[:, None] * jnp.maximum(similar - cover[:, None], 0.0), axis=0) * weight / total)
        column = lax.dynamic_index_in_dim(similar, class_picks[turn_index].astype(jnp.int32), 1, keepdims=False)
        cover = jnp.maximum(cover, column)
    return jnp.stack(scores), cover * weight


def score_item(packed):
    return class_scores(packed[0], packed[1], packed[2])


def reference(sketches, labels, places, counts, chosen):
    flat_index = (labels * BLOCK + places).astype(jnp.int32)
    blocks = jnp.zeros((CLASSES * BLOCK, D), sketches.dtype).at[flat_index].set(sketches)
    blocks = blocks.reshape(CLASSES, BLOCK, D)
    scores, cover = lax.map(score_item, (blocks, counts, jnp.transpose(chosen)))
    return jnp.transpose(scores, (1, 0, 2)), cover
```

```python
import functools

import jax
import jax.numpy as jnp
from jax import lax
from jax.experimental import pallas as pl
from jax.experimental.pallas import tpu as pltpu
from jax.sharding import PartitionSpec as P

MESH = pl.DeviceIdType.MESH
UNIT = 16
PICK_ROWS = 16
PARTS = 8
WINDOW = 3
FAR = 1e30


def ring_place(index):
    high = index // 2
    return 2 * high + (index % 2 + high) % 2


def ring_member(place):
    high = place // 2
    return 2 * high + (place % 2 + high) % 2


def dot_rows(left, right):
    return lax.dot_general(
        left, right, (((1,), (1,)), ((), ())), preferred_element_type=jnp.float32
    )


def class_kernel(
    members,
    owners,
    sub,
    steps,
    target_ref,
    pick_ref,
    counts_ref,
    sketch_ref,
    result_ref,
    table_ref,
    out_ref,
    rows_ref,
    picks_ref,
    inner_ref,
    pick_inner_ref,
    squares_ref,
    pick_squares_ref,
    bound_ref,
    wide_ref,
    row_gain_ref,
    gains_ref,
    final_ref,
    a_send,
    a_recv,
    b_send,
    b_recv,
    p_send,
    p_recv,
    m_send,
    m_recv,
    g_send,
    g_recv,
):
    member = lax.axis_index("dp")
    owner = lax.axis_index("cls")
    row_count, width = sketch_ref.shape
    parts, part = out_ref.shape[0], out_ref.shape[-1]
    chunks = rows_ref.shape[2]
    lanes = owners * UNIT
    capacity = chunks * lanes
    half = members // 2
    slots = half + 1
    window = min(WINDOW, parts - 1)
    place = ring_place(member)
    step = 1 - 2 * (owner % 2)
    sends_half = (place // half + owner % 2) % 2 == 0
    gets_half = (place // half + owner % 2) % 2 == 1
    scale = 1.0 / width

    barrier = pltpu.get_barrier_semaphore()
    for hop in range(1, owners):
        pl.semaphore_signal(
            barrier, inc=1, device_id=(member, (owner + hop) % owners), device_id_type=MESH
        )
    for hop in range(1, members):
        pl.semaphore_signal(
            barrier,
            inc=1,
            device_id=(ring_member((place + hop) % members), owner),
            device_id_type=MESH,
        )

    def dispatch(f, hop):
        target = (owner + hop) % owners
        return pltpu.make_async_remote_copy(
            src_ref=out_ref.at[f, target],
            dst_ref=rows_ref.at[0, f, :, owner],
            send_sem=a_send.at[f, hop - 1],
            recv_sem=a_recv.at[f, hop - 1],
            device_id=(member, target),
            device_id_type=MESH,
        )

    def share(f, hop):
        target = ring_member((place + step * hop + members) % members)
        return pltpu.make_async_remote_copy(
            src_ref=rows_ref.at[0, f],
            dst_ref=rows_ref.at[hop, f],
            send_sem=b_send.at[f, hop - 1],
            recv_sem=b_recv.at[f, hop - 1],
            device_id=(target, owner),
            device_id_type=MESH,
        )

    def share_picks(f, hop):
        return pltpu.make_async_remote_copy(
            src_ref=picks_ref.at[0, f],
            dst_ref=picks_ref.at[hop, f],
            send_sem=p_send.at[f, hop - 1],
            recv_sem=p_recv.at[f, hop - 1],
            device_id=(ring_member((place + hop) % members), owner),
            device_id_type=MESH,
        )

    def share_bound(hop):
        return pltpu.make_async_remote_copy(
            src_ref=bound_ref.at[0],
            dst_ref=bound_ref.at[hop],
            send_sem=m_send.at[hop - 1],
            recv_sem=m_recv.at[hop - 1],
            device_id=(ring_member((place + hop) % members), owner),
            device_id_type=MESH,
        )

    def share_gains(hop):
        target = ring_member((place + hop) % members)
        return pltpu.make_async_remote_copy(
            src_ref=gains_ref.at[target * sub // UNIT],
            dst_ref=final_ref.at[members - hop],
            send_sem=g_send.at[hop - 1],
            recv_sem=g_recv.at[hop - 1],
            device_id=(target, owner),
            device_id_type=MESH,
        )

    def prepare(f):
        low = pl.multiple_of(f * part, part)
        block = jnp.dot(
            table_ref[...],
            sketch_ref[:, pl.ds(low, part)],
            preferred_element_type=jnp.float32,
        ).astype(out_ref.dtype)
        out_ref[f] = block.reshape(out_ref.shape[1:])
        rows_ref[0, f, :, owner] = out_ref[f, owner]

    def part_rows(slot, f):
        return rows_ref[slot, f].reshape(capacity, part)

    def multiply(slot, f):
        block = part_rows(slot, f)
        product = dot_rows(part_rows(0, f), block)
        for chunk in range(chunks):
            inner_ref[slot * chunks + chunk] += product[:, chunk * lanes : (chunk + 1) * lanes]
        total = jnp.zeros((capacity, 128), jnp.float32)
        for low in range(0, part, 128):
            wide = block[:, low : low + 128].astype(jnp.float32)
            total = total + wide * wide
        squares_ref[slot] += total

    def multiply_picks(slot, f, picks):
        pick_inner_ref[slot] += dot_rows(picks, part_rows(slot, f))

    def own_part(f):
        picks_ref[0, f] = lax.dot_general(
            pick_table,
            part_rows(0, f),
            (((1,), (0,)), ((), ())),
            preferred_element_type=jnp.float32,
        ).astype(picks_ref.dtype)
        multiply(0, f)
        for hop in range(1, members):
            share_picks(f, hop).start()

    def other_part(f):
        for hop in range(1, members):
            share_picks(f, hop).wait_recv()
        picks = picks_ref[0, f].astype(jnp.float32)
        for hop in range(1, members):
            picks = picks + picks_ref[hop, f].astype(jnp.float32)
        total = jnp.zeros((PICK_ROWS, 128), jnp.float32)
        for low in range(0, part, 128):
            wide = picks[:, low : low + 128]
            total = total + wide * wide
        pick_squares_ref[...] += total
        picks = picks.astype(picks_ref.dtype)
        multiply_picks(0, f, picks)
        for hop in range(1, half):
            share(f, hop).wait_recv()
            multiply(hop, f)
            multiply_picks(hop, f, picks)

        @pl.when(gets_half)
        def _():
            share(f, half).wait_recv()
            multiply(half, f)
            multiply_picks(half, f, picks)

    table_ref[...] = (
        lax.broadcasted_iota(jnp.int32, (2 * row_count, row_count), 0) == target_ref[...]
    ).astype(table_ref.dtype)
    for f in range(window + 1):
        prepare(f)
    pl.semaphore_wait(barrier, owners + members - 2)
    for f in range(window):
        for hop in range(1, owners):
            dispatch(f, hop).start()

    inner_ref[...] = jnp.zeros_like(inner_ref)
    pick_inner_ref[...] = jnp.zeros_like(pick_inner_ref)
    squares_ref[...] = jnp.zeros_like(squares_ref)
    pick_squares_ref[...] = jnp.zeros_like(pick_squares_ref)
    pick_table = (
        lax.broadcasted_iota(jnp.int32, (PICK_ROWS, capacity), 1) + member * capacity
        == pick_ref[:, :1]
    ).astype(rows_ref.dtype)

    @pl.loop(0, parts)
    def _(f):
        for hop in range(1, owners):
            dispatch(f, hop).wait_recv()

        @pl.when(sends_half)
        def _():
            share(f, half).start()

        for hop in range(1, half):
            share(f, hop).start()

        @pl.when(f + window < parts)
        def _():
            for hop in range(1, owners):
                dispatch(f + window, hop).start()

        @pl.when(f + window + 1 < parts)
        def _():
            prepare(f + window + 1)

        own_part(f)

        @pl.when(f > 0)
        def _():
            other_part(f - 1)

    other_part(parts - 1)

    lane = lax.broadcasted_iota(jnp.int32, (members * owners, lanes), 1)
    source = lax.broadcasted_iota(jnp.int32, (members * owners, lanes), 0)
    spot = lax.broadcasted_iota(jnp.int32, (1, lanes), 1) & (sub - 1)
    lows = UNIT // sub
    unit_bits = UNIT.bit_length() - 1
    sub_bits = sub.bit_length() - 1

    def valid_row(slot):
        block = ring_member((place - step * slot + members) % members)
        filled = jnp.zeros((chunks, lanes), jnp.float32)
        for low in range(lows):
            spread_out = (source == block * owners + (lane >> unit_bits)) & (
                ((lane >> sub_bits) & (lows - 1)) == low
            )
            filled = filled + jnp.dot(
                counts_ref[low].astype(jnp.float32).astype(jnp.bfloat16),
                spread_out.astype(jnp.bfloat16),
                preferred_element_type=jnp.float32,
            )
        row = filled > spot.astype(jnp.float32)
        if slot == half:
            row = row & gets_half
        row = row.astype(jnp.float32)
        return jnp.concatenate([row[chunk : chunk + 1] for chunk in range(chunks)], axis=1)

    def turned(row):
        return jnp.transpose(jnp.broadcast_to(row, (128, capacity)))

    valid = [valid_row(slot) > 0.5 for slot in range(slots)]
    norm = [
        jnp.sum(jnp.transpose(squares_ref[slot]), axis=0, keepdims=True) * scale
        for slot in range(slots)
    ]
    pick_norm = jnp.sum(pick_squares_ref[...], axis=1, keepdims=True) * scale

    wide_ref[0] = turned(jnp.where(valid[0], norm[0], -FAR))
    near = wide_ref[0]
    if lanes > 128:
        near = jnp.concatenate([near] * (lanes // 128), axis=1)
    largest = jnp.zeros((1, lanes), jnp.float32)
    for slot in range(slots):
        for chunk in range(chunks):
            cut = slice(chunk * lanes, (chunk + 1) * lanes)
            tile = jnp.max(
                near - (2.0 * scale) * inner_ref[slot * chunks + chunk], axis=0, keepdims=True
            )
            tile = jnp.where(valid[slot][:, cut], tile + norm[slot][:, cut], 0.0)
            largest = jnp.maximum(largest, tile)
    bound_ref[0] = jnp.broadcast_to(jnp.max(largest, axis=1, keepdims=True), bound_ref.shape[1:])
    for hop in range(1, members):
        share_bound(hop).start()
    for hop in range(1, members):
        share_bound(hop).wait_recv()
    bound = bound_ref[0]
    for hop in range(1, members):
        bound = jnp.maximum(bound, bound_ref[hop])
    bound = bound[:1, :1]

    covers = []
    for slot in range(slots):
        cover = jnp.zeros((1, capacity), jnp.float32)
        held = [cover]
        for turn in range(steps):
            similar = bound - (
                pick_norm[turn : turn + 1]
                + norm[slot]
                - (2.0 * scale) * pick_inner_ref[slot][turn : turn + 1]
            )
            cover = jnp.maximum(cover, similar)
            held.append(cover)
        covers.append(held)

    for turn in range(steps):
        wide_ref[turn] = turned(
            jnp.where(valid[0], bound - norm[0] - covers[0][turn], -FAR)
        )
    row_gain_ref[...] = jnp.zeros_like(row_gain_ref)
    open_near = turned(bound - norm[0])
    wide_ref[steps] = open_near

    def repeat(block):
        if lanes > 128:
            block = jnp.concatenate([block] * (lanes // 128), axis=1)
        return block

    for slot in range(slots):
        for chunk in range(chunks):
            cut = slice(chunk * lanes, (chunk + 1) * lanes)
            tile = (2.0 * scale) * inner_ref[slot * chunks + chunk] - norm[slot][:, cut]
            gained = []
            for turn in range(steps):
                gained.append(
                    jnp.sum(
                        jnp.maximum(tile + repeat(wide_ref[turn]), 0.0), axis=0, keepdims=True
                    )
                )
                if slot > 0:
                    far = jnp.where(valid[slot][:, cut], covers[slot][turn][:, cut], FAR)
                    each = jnp.maximum(tile + repeat(wide_ref[steps]) - far, 0.0)
                    for low in range(0, lanes, 128):
                        row_gain_ref[turn] += each[:, low : low + 128]
            if slot == half:
                gained = [jnp.where(gets_half, row, 0.0) for row in gained]
            last = covers[0][steps][:, cut] if slot == 0 else jnp.zeros((1, lanes), jnp.float32)
            blank = jnp.zeros((8 - steps - 1, lanes), jnp.float32)
            gains_ref[chunk, slot] = jnp.concatenate([*gained, last, blank], axis=0)
    for turn in range(steps):
        row = jnp.sum(jnp.transpose(row_gain_ref[turn]), axis=0, keepdims=True)
        for chunk in range(chunks):
            gains_ref[chunk, 0, turn : turn + 1] += row[:, chunk * lanes : (chunk + 1) * lanes]

    for hop in range(1, members):
        share_gains(hop).start()
    final_ref[0] = gains_ref[member * sub // UNIT]
    for hop in range(1, members):
        share_gains(hop).wait_recv()
    for ahead in range(members):
        summed = final_ref[ahead, 0]
        for slot in range(1, slots):
            summed = summed + final_ref[(ahead + step * slot + members) % members, slot]
        block = ring_member((place + ahead) % members)
        result_ref[:, pl.ds(pl.multiple_of(block * lanes, lanes), lanes)] = summed

    @pl.loop(0, parts)
    def _(f):
        for hop in range(1, owners):
            dispatch(f, hop).wait_send()
        for hop in range(1, half):
            share(f, hop).wait_send()
        for hop in range(1, members):
            share_picks(f, hop).wait_send()

        @pl.when(sends_half)
        def _():
            share(f, half).wait_send()

    for hop in range(1, members):
        share_bound(hop).wait_send()
        share_gains(hop).wait_send()


def class_gains(target, picks, counts, sketches, members, owners, sub, steps):
    row_count, width = sketches.shape
    chunks = members * sub // UNIT
    lanes = owners * UNIT
    capacity = chunks * lanes
    slots = members // 2 + 1
    part = width // PARTS
    kind = sketches.dtype
    vmem = pl.BlockSpec(memory_space=pltpu.VMEM)
    dma = pltpu.SemaphoreType.DMA
    return pl.pallas_call(
        functools.partial(class_kernel, members, owners, sub, steps),
        out_shape=jax.ShapeDtypeStruct((8, members * lanes), jnp.float32),
        in_specs=[vmem, vmem, vmem, vmem],
        out_specs=vmem,
        scratch_shapes=[
            pltpu.VMEM((2 * row_count, row_count), kind),
            pltpu.VMEM((PARTS, owners, chunks, UNIT, part), kind),
            pltpu.VMEM((slots, PARTS, chunks, owners, UNIT, part), kind),
            pltpu.VMEM((members, PARTS, PICK_ROWS, part), kind),
            pltpu.VMEM((slots * chunks, capacity, lanes), jnp.float32),
            pltpu.VMEM((slots, PICK_ROWS, capacity), jnp.float32),
            pltpu.VMEM((slots, capacity, 128), jnp.float32),
            pltpu.VMEM((PICK_ROWS, 128), jnp.float32),
            pltpu.VMEM((members, 8, 128), jnp.float32),
            pltpu.VMEM((steps + 1, capacity, 128), jnp.float32),
            pltpu.VMEM((steps, capacity, 128), jnp.float32),
            pltpu.VMEM((chunks, slots, 8, lanes), jnp.float32),
            pltpu.VMEM((members, slots, 8, lanes), jnp.float32),
            dma((PARTS, owners - 1)),
            dma((PARTS, owners - 1)),
            dma((PARTS, members // 2)),
            dma((PARTS, members // 2)),
            dma((PARTS, members - 1)),
            dma((PARTS, members - 1)),
            dma((members - 1,)),
            dma((members - 1,)),
            dma((members - 1,)),
            dma((members - 1,)),
        ],
        compiler_params=pltpu.CompilerParams(
            collective_id=0, has_side_effects=True, vmem_limit_bytes=60 * 1024 * 1024
        ),
    )(target, picks, counts, sketches)


def body(sketches, labels, places, counts, chosen):
    row_count = sketches.shape[0]
    members = lax.axis_size("dp")
    owners = lax.axis_size("cls")
    devices = members * owners
    sub = 2 * row_count // devices
    capacity = devices * sub
    chunks = members * sub // UNIT
    lows = UNIT // sub
    member = lax.axis_index("dp")
    steps = chosen.shape[0]

    target = (labels * members + places // capacity) * sub + places % sub
    source = chosen % capacity // sub
    offset = chosen // capacity * sub + chosen % sub
    pick = (offset // UNIT * owners + source % owners) * UNIT + offset % UNIT
    pick = jnp.pad(
        source // owners * capacity + pick, ((0, PICK_ROWS - steps), (0, 127)), constant_values=-1
    )
    class_counts = counts[0]
    filled = jnp.transpose(class_counts.reshape(chunks, lows, devices), (1, 0, 2))

    result = class_gains(
        target.reshape(1, row_count), pick, filled, sketches, members, owners, sub, steps
    )
    total = jnp.sum(class_counts).astype(jnp.float32)
    if lows > 1:
        result = lax.dynamic_index_in_dim(
            result.reshape(8, members * owners, lows, sub), member % lows, 2, False
        ).reshape(8, capacity)
    mine = lax.dynamic_index_in_dim(class_counts, member, 0, False)
    spot = lax.broadcasted_iota(jnp.int32, (devices, sub), 1)
    place_valid = (spot < mine[:, None]).reshape(capacity).astype(jnp.float32)
    gain_scores = (result[:steps] * place_valid[None, :] / total)[:, None, :]
    coverage = (result[steps] * place_valid)[None, :]
    return (gain_scores, coverage)


def solution(mesh):
    placed = (
        P(("dp", "cls"), None),
        P(("dp", "cls")),
        P(("dp", "cls")),
        P("cls", None, None),
        P(None, "cls"),
    )
    return jax.shard_map(
        body,
        mesh=mesh,
        in_specs=placed,
        out_specs=(P(None, "cls", "dp"), P("cls", "dp")),
        check_vma=False,
    )
```

```python
import functools

import jax
import jax.numpy as jnp
from jax import lax
from jax.experimental import pallas as pl
from jax.experimental.pallas import tpu as pltpu
from jax.sharding import PartitionSpec as P

MESH = pl.DeviceIdType.MESH
UNIT = 16
PICK_ROWS = 16
PARTS = 8
WINDOW = 2
FAR = 1e30


def ring_place(index):
    high = index // 2
    return 2 * high + (index % 2 + high) % 2


def ring_member(place):
    high = place // 2
    return 2 * high + (place % 2 + high) % 2


def dot_rows(left, right):
    return lax.dot_general(
        left, right, (((1,), (1,)), ((), ())), preferred_element_type=jnp.float32
    )


def class_kernel(
    members,
    owners,
    sub,
    steps,
    target_ref,
    pick_ref,
    counts_ref,
    sketch_ref,
    result_ref,
    table_ref,
    out_ref,
    rows_ref,
    picks_ref,
    inner_ref,
    pick_inner_ref,
    squares_ref,
    pick_squares_ref,
    bound_ref,
    wide_ref,
    row_gain_ref,
    gains_ref,
    final_ref,
    a_send,
    a_recv,
    b_send,
    b_recv,
    x_send,
    x_recv,
    p_send,
    p_recv,
    m_send,
    m_recv,
    g_send,
    g_recv,
):
    member = lax.axis_index("dp")
    owner = lax.axis_index("cls")
    row_count, width = sketch_ref.shape
    parts, part = out_ref.shape[0], out_ref.shape[-1]
    chunks = rows_ref.shape[2]
    lanes = owners * UNIT
    capacity = chunks * lanes
    half = members // 2
    slots = half + 1
    window = min(WINDOW, parts - 1)
    place = ring_place(member)
    step = 1 - 2 * (owner % 2)
    ring = (step * place + members) % members
    cut_chunk = chunks // 2
    gets_first = ring < half
    gets_second = (ring >= 1) & (ring <= half)
    gives_first = (ring + 1) % members < half
    gives_second = ring >= half
    scale = 1.0 / width

    barrier = pltpu.get_barrier_semaphore()
    for hop in range(1, owners):
        pl.semaphore_signal(
            barrier, inc=1, device_id=(member, (owner + hop) % owners), device_id_type=MESH
        )
    for hop in range(1, members):
        pl.semaphore_signal(
            barrier,
            inc=1,
            device_id=(ring_member((place + hop) % members), owner),
            device_id_type=MESH,
        )

    def dispatch(f, hop):
        target = (owner + hop) % owners
        return pltpu.make_async_remote_copy(
            src_ref=out_ref.at[f, target],
            dst_ref=rows_ref.at[0, f, :, owner],
            send_sem=a_send.at[f, hop - 1],
            recv_sem=a_recv.at[f, hop - 1],
            device_id=(member, target),
            device_id_type=MESH,
        )

    def share(f, hop):
        target = ring_member((place + step * hop + members) % members)
        return pltpu.make_async_remote_copy(
            src_ref=rows_ref.at[0, f],
            dst_ref=rows_ref.at[hop, f],
            send_sem=b_send.at[f, hop - 1],
            recv_sem=b_recv.at[f, hop - 1],
            device_id=(target, owner),
            device_id_type=MESH,
        )

    def share_first(f):
        return pltpu.make_async_remote_copy(
            src_ref=rows_ref.at[half - 1, f, :cut_chunk],
            dst_ref=rows_ref.at[half, f, :cut_chunk],
            send_sem=x_send.at[f, 0],
            recv_sem=x_recv.at[f, 0],
            device_id=(ring_member((place + step + members) % members), owner),
            device_id_type=MESH,
        )

    def share_second(f):
        target = ring_member((place + step * (half + 1) + members * half) % members)
        return pltpu.make_async_remote_copy(
            src_ref=rows_ref.at[0, f, cut_chunk:],
            dst_ref=rows_ref.at[half, f, cut_chunk:],
            send_sem=x_send.at[f, 1],
            recv_sem=x_recv.at[f, 1],
            device_id=(target, owner),
            device_id_type=MESH,
        )

    def share_picks(f, hop):
        return pltpu.make_async_remote_copy(
            src_ref=picks_ref.at[0, f],
            dst_ref=picks_ref.at[hop, f],
            send_sem=p_send.at[f, hop - 1],
            recv_sem=p_recv.at[f, hop - 1],
            device_id=(ring_member((place + hop) % members), owner),
            device_id_type=MESH,
        )

    def share_bound(hop):
        return pltpu.make_async_remote_copy(
            src_ref=bound_ref.at[0],
            dst_ref=bound_ref.at[hop],
            send_sem=m_send.at[hop - 1],
            recv_sem=m_recv.at[hop - 1],
            device_id=(ring_member((place + hop) % members), owner),
            device_id_type=MESH,
        )

    def share_gains(hop):
        target = ring_member((place + hop) % members)
        return pltpu.make_async_remote_copy(
            src_ref=gains_ref.at[target * sub // UNIT],
            dst_ref=final_ref.at[members - hop],
            send_sem=g_send.at[hop - 1],
            recv_sem=g_recv.at[hop - 1],
            device_id=(target, owner),
            device_id_type=MESH,
        )

    def prepare(f):
        low = pl.multiple_of(f * part, part)
        block = jnp.dot(
            table_ref[...],
            sketch_ref[:, pl.ds(low, part)],
            preferred_element_type=jnp.float32,
        ).astype(out_ref.dtype)
        out_ref[f] = block.reshape(out_ref.shape[1:])
        rows_ref[0, f, :, owner] = out_ref[f, owner]

    def part_rows(slot, f):
        return rows_ref[slot, f].reshape(capacity, part)

    def multiply(slot, f, left=0, first=0, last=chunks):
        low, high = first * lanes, last * lanes
        block = rows_ref[slot, f, first:last].reshape(high - low, part)
        product = dot_rows(part_rows(left, f), block)
        for chunk in range(first, last):
            cut = slice(chunk * lanes - low, (chunk + 1) * lanes - low)
            inner_ref[slot * chunks + chunk] += product[:, cut]
        total = jnp.zeros((high - low, 128), jnp.float32)
        for spot in range(0, part, 128):
            wide = block[:, spot : spot + 128].astype(jnp.float32)
            total = total + wide * wide
        squares_ref[slot, low:high] += total

    def multiply_picks(slot, f, picks, first=0, last=chunks):
        low, high = first * lanes, last * lanes
        block = rows_ref[slot, f, first:last].reshape(high - low, part)
        pick_inner_ref[slot, :, low:high] += dot_rows(picks, block)

    def own_part(f):
        picks_ref[0, f] = lax.dot_general(
            pick_table,
            part_rows(0, f),
            (((1,), (0,)), ((), ())),
            preferred_element_type=jnp.float32,
        ).astype(picks_ref.dtype)
        multiply(0, f)
        for hop in range(1, members):
            share_picks(f, hop).start()

    def other_part(f):
        for hop in range(1, half):
            share(f, hop).wait_recv()

        @pl.when(gives_first)
        def _():
            share_first(f).start()

        for hop in range(1, members):
            share_picks(f, hop).wait_recv()
        picks = picks_ref[0, f].astype(jnp.float32)
        for hop in range(1, members):
            picks = picks + picks_ref[hop, f].astype(jnp.float32)
        total = jnp.zeros((PICK_ROWS, 128), jnp.float32)
        for low in range(0, part, 128):
            wide = picks[:, low : low + 128]
            total = total + wide * wide
        pick_squares_ref[...] += total
        picks = picks.astype(picks_ref.dtype)
        multiply_picks(0, f, picks)
        for hop in range(1, half):
            multiply(hop, f)
            multiply_picks(hop, f, picks)

        @pl.when(gets_second)
        def _():
            share_second(f).wait_recv()
            multiply(half, f, 1, cut_chunk, chunks)
            multiply_picks(half, f, picks, cut_chunk, chunks)

        @pl.when(gets_first)
        def _():
            share_first(f).wait_recv()
            multiply(half, f, 0, 0, cut_chunk)
            multiply_picks(half, f, picks, 0, cut_chunk)

    table_ref[...] = (
        lax.broadcasted_iota(jnp.int32, (2 * row_count, row_count), 0) == target_ref[...]
    ).astype(table_ref.dtype)
    for f in range(window + 1):
        prepare(f)
    pl.semaphore_wait(barrier, owners + members - 2)
    for f in range(window):
        for hop in range(1, owners):
            dispatch(f, hop).start()

    inner_ref[...] = jnp.zeros_like(inner_ref)
    pick_inner_ref[...] = jnp.zeros_like(pick_inner_ref)
    squares_ref[...] = jnp.zeros_like(squares_ref)
    pick_squares_ref[...] = jnp.zeros_like(pick_squares_ref)
    pick_table = (
        lax.broadcasted_iota(jnp.int32, (PICK_ROWS, capacity), 1) + member * capacity
        == pick_ref[:, :1]
    ).astype(rows_ref.dtype)

    @pl.loop(0, parts)
    def _(f):
        for hop in range(1, owners):
            dispatch(f, hop).wait_recv()

        for hop in range(1, half):
            share(f, hop).start()

        @pl.when(gives_second)
        def _():
            share_second(f).start()

        @pl.when(f + window < parts)
        def _():
            for hop in range(1, owners):
                dispatch(f + window, hop).start()

        @pl.when(f + window + 1 < parts)
        def _():
            prepare(f + window + 1)

        own_part(f)

        @pl.when(f > 0)
        def _():
            other_part(f - 1)

    other_part(parts - 1)

    lane = lax.broadcasted_iota(jnp.int32, (members * owners, lanes), 1)
    source = lax.broadcasted_iota(jnp.int32, (members * owners, lanes), 0)
    spot = lax.broadcasted_iota(jnp.int32, (1, lanes), 1) & (sub - 1)
    lows = UNIT // sub
    unit_bits = UNIT.bit_length() - 1
    sub_bits = sub.bit_length() - 1

    def block_row(behind):
        block = ring_member((place - step * behind + members * half) % members)
        filled = jnp.zeros((chunks, lanes), jnp.float32)
        for low in range(lows):
            spread_out = (source == block * owners + (lane >> unit_bits)) & (
                ((lane >> sub_bits) & (lows - 1)) == low
            )
            filled = filled + jnp.dot(
                counts_ref[low].astype(jnp.float32).astype(jnp.bfloat16),
                spread_out.astype(jnp.bfloat16),
                preferred_element_type=jnp.float32,
            )
        row = (filled > spot.astype(jnp.float32)).astype(jnp.float32)
        return jnp.concatenate([row[chunk : chunk + 1] for chunk in range(chunks)], axis=1)

    def valid_row(slot):
        if slot < half:
            return block_row(slot)
        split = cut_chunk * lanes
        first = jnp.where(gets_first, block_row(half)[:, :split], 0.0)
        second = jnp.where(gets_second, block_row(half + 1)[:, split:], 0.0)
        return jnp.concatenate([first, second], axis=1)

    def turned(row):
        return jnp.transpose(jnp.broadcast_to(row, (128, capacity)))

    valid = [valid_row(slot) > 0.5 for slot in range(slots)]
    norm = [
        jnp.sum(jnp.transpose(squares_ref[slot]), axis=0, keepdims=True) * scale
        for slot in range(slots)
    ]
    pick_norm = jnp.sum(pick_squares_ref[...], axis=1, keepdims=True) * scale

    def repeat(block):
        if lanes > 128:
            block = jnp.concatenate([block] * (lanes // 128), axis=1)
        return block

    def left_of(slot, chunk):
        return 1 if slot == half and chunk >= cut_chunk else 0

    for left in range(2):
        wide_ref[left, 0] = turned(jnp.where(valid[left], norm[left], -FAR))
    largest = jnp.zeros((1, lanes), jnp.float32)
    for slot in range(slots):
        for chunk in range(chunks):
            cut = slice(chunk * lanes, (chunk + 1) * lanes)
            near = repeat(wide_ref[left_of(slot, chunk), 0])
            tile = jnp.max(
                near - (2.0 * scale) * inner_ref[slot * chunks + chunk], axis=0, keepdims=True
            )
            tile = jnp.where(valid[slot][:, cut], tile + norm[slot][:, cut], 0.0)
            largest = jnp.maximum(largest, tile)
    bound_ref[0] = jnp.broadcast_to(jnp.max(largest, axis=1, keepdims=True), bound_ref.shape[1:])
    for hop in range(1, members):
        share_bound(hop).start()
    for hop in range(1, members):
        share_bound(hop).wait_recv()
    bound = bound_ref[0]
    for hop in range(1, members):
        bound = jnp.maximum(bound, bound_ref[hop])
    bound = bound[:1, :1]

    covers = []
    for slot in range(slots):
        cover = jnp.zeros((1, capacity), jnp.float32)
        held = [cover]
        for turn in range(steps):
            similar = bound - (
                pick_norm[turn : turn + 1]
                + norm[slot]
                - (2.0 * scale) * pick_inner_ref[slot][turn : turn + 1]
            )
            cover = jnp.maximum(cover, similar)
            held.append(cover)
        covers.append(held)

    for left in range(2):
        for turn in range(steps):
            wide_ref[left, turn] = turned(
                jnp.where(valid[left], bound - norm[left] - covers[left][turn], -FAR)
            )
        wide_ref[left, steps] = turned(bound - norm[left])
    row_gain_ref[...] = jnp.zeros_like(row_gain_ref)

    for slot in range(slots):
        for chunk in range(chunks):
            cut = slice(chunk * lanes, (chunk + 1) * lanes)
            tile = (2.0 * scale) * inner_ref[slot * chunks + chunk] - norm[slot][:, cut]
            gained = []
            left = left_of(slot, chunk)
            for turn in range(steps):
                gained.append(
                    jnp.sum(
                        jnp.maximum(tile + repeat(wide_ref[left, turn]), 0.0),
                        axis=0,
                        keepdims=True,
                    )
                )
                if slot > 0:
                    far = jnp.where(valid[slot][:, cut], covers[slot][turn][:, cut], FAR)
                    each = jnp.maximum(tile + repeat(wide_ref[left, steps]) - far, 0.0)
                    for low in range(0, lanes, 128):
                        row_gain_ref[left, turn] += each[:, low : low + 128]
            if slot == half:
                gets = gets_second if left else gets_first
                gained = [jnp.where(gets, row, 0.0) for row in gained]
            last = covers[0][steps][:, cut] if slot == 0 else jnp.zeros((1, lanes), jnp.float32)
            blank = jnp.zeros((8 - steps - 1, lanes), jnp.float32)
            gains_ref[chunk, slot] = jnp.concatenate([*gained, last, blank], axis=0)
    for left in range(2):
        for turn in range(steps):
            row = jnp.sum(jnp.transpose(row_gain_ref[left, turn]), axis=0, keepdims=True)
            for chunk in range(chunks):
                cut = slice(chunk * lanes, (chunk + 1) * lanes)
                gains_ref[chunk, left, turn : turn + 1] += row[:, cut]

    for hop in range(1, members):
        share_gains(hop).start()
    final_ref[0] = gains_ref[member * sub // UNIT]
    for hop in range(1, members):
        share_gains(hop).wait_recv()
    second = (member * sub // UNIT) // cut_chunk
    for ahead in range(members):
        summed = final_ref[ahead, 0]
        for slot in range(1, slots):
            behind = slot if slot < half else half + second
            holder = (ahead + step * behind + members * half) % members
            summed = summed + final_ref[holder, slot]
        block = ring_member((place + ahead) % members)
        result_ref[:, pl.ds(pl.multiple_of(block * lanes, lanes), lanes)] = summed

    @pl.loop(0, parts)
    def _(f):
        for hop in range(1, owners):
            dispatch(f, hop).wait_send()
        for hop in range(1, half):
            share(f, hop).wait_send()
        for hop in range(1, members):
            share_picks(f, hop).wait_send()

        @pl.when(gives_second)
        def _():
            share_second(f).wait_send()

        @pl.when(gives_first)
        def _():
            share_first(f).wait_send()

    for hop in range(1, members):
        share_bound(hop).wait_send()
        share_gains(hop).wait_send()


def class_gains(target, picks, counts, sketches, members, owners, sub, steps):
    row_count, width = sketches.shape
    chunks = members * sub // UNIT
    lanes = owners * UNIT
    capacity = chunks * lanes
    slots = members // 2 + 1
    part = width // PARTS
    kind = sketches.dtype
    vmem = pl.BlockSpec(memory_space=pltpu.VMEM)
    dma = pltpu.SemaphoreType.DMA
    return pl.pallas_call(
        functools.partial(class_kernel, members, owners, sub, steps),
        out_shape=jax.ShapeDtypeStruct((8, members * lanes), jnp.float32),
        in_specs=[vmem, vmem, vmem, vmem],
        out_specs=vmem,
        scratch_shapes=[
            pltpu.VMEM((2 * row_count, row_count), kind),
            pltpu.VMEM((PARTS, owners, chunks, UNIT, part), kind),
            pltpu.VMEM((slots, PARTS, chunks, owners, UNIT, part), kind),
            pltpu.VMEM((members, PARTS, PICK_ROWS, part), kind),
            pltpu.VMEM((slots * chunks, capacity, lanes), jnp.float32),
            pltpu.VMEM((slots, PICK_ROWS, capacity), jnp.float32),
            pltpu.VMEM((slots, capacity, 128), jnp.float32),
            pltpu.VMEM((PICK_ROWS, 128), jnp.float32),
            pltpu.VMEM((members, 8, 128), jnp.float32),
            pltpu.VMEM((2, steps + 1, capacity, 128), jnp.float32),
            pltpu.VMEM((2, steps, capacity, 128), jnp.float32),
            pltpu.VMEM((chunks, slots, 8, lanes), jnp.float32),
            pltpu.VMEM((members, slots, 8, lanes), jnp.float32),
            dma((PARTS, owners - 1)),
            dma((PARTS, owners - 1)),
            dma((PARTS, members // 2 - 1)),
            dma((PARTS, members // 2 - 1)),
            dma((PARTS, 2)),
            dma((PARTS, 2)),
            dma((PARTS, members - 1)),
            dma((PARTS, members - 1)),
            dma((members - 1,)),
            dma((members - 1,)),
            dma((members - 1,)),
            dma((members - 1,)),
        ],
        compiler_params=pltpu.CompilerParams(
            collective_id=0, has_side_effects=True, vmem_limit_bytes=60 * 1024 * 1024
        ),
    )(target, picks, counts, sketches)


def body(sketches, labels, places, counts, chosen):
    row_count = sketches.shape[0]
    members = lax.axis_size("dp")
    owners = lax.axis_size("cls")
    devices = members * owners
    sub = 2 * row_count // devices
    capacity = devices * sub
    chunks = members * sub // UNIT
    lows = UNIT // sub
    member = lax.axis_index("dp")
    steps = chosen.shape[0]

    target = (labels * members + places // capacity) * sub + places % sub
    source = chosen % capacity // sub
    offset = chosen // capacity * sub + chosen % sub
    pick = (offset // UNIT * owners + source % owners) * UNIT + offset % UNIT
    pick = jnp.pad(
        source // owners * capacity + pick, ((0, PICK_ROWS - steps), (0, 127)), constant_values=-1
    )
    class_counts = counts[0]
    filled = jnp.transpose(class_counts.reshape(chunks, lows, devices), (1, 0, 2))

    result = class_gains(
        target.reshape(1, row_count), pick, filled, sketches, members, owners, sub, steps
    )
    total = jnp.sum(class_counts).astype(jnp.float32)
    if lows > 1:
        result = lax.dynamic_index_in_dim(
            result.reshape(8, members * owners, lows, sub), member % lows, 2, False
        ).reshape(8, capacity)
    mine = lax.dynamic_index_in_dim(class_counts, member, 0, False)
    spot = lax.broadcasted_iota(jnp.int32, (devices, sub), 1)
    place_valid = (spot < mine[:, None]).reshape(capacity).astype(jnp.float32)
    gain_scores = (result[:steps] * place_valid[None, :] / total)[:, None, :]
    coverage = (result[steps] * place_valid)[None, :]
    return (gain_scores, coverage)


def solution(mesh):
    placed = (
        P(("dp", "cls"), None),
        P(("dp", "cls")),
        P(("dp", "cls")),
        P("cls", None, None),
        P(None, "cls"),
    )
    return jax.shard_map(
        body,
        mesh=mesh,
        in_specs=placed,
        out_specs=(P(None, "cls", "dp"), P("cls", "dp")),
        check_vma=False,
    )
```

```python
import functools

import jax
import jax.numpy as jnp
from jax import lax
from jax.experimental import pallas as pl
from jax.experimental.pallas import tpu as pltpu
from jax.sharding import PartitionSpec as P

MESH = pl.DeviceIdType.MESH
UNIT = 16
PICK_ROWS = 16
PARTS = 16
WINDOW = 2
FAR = 1e30


def ring_place(index):
    high = index // 2
    return 2 * high + (index % 2 + high) % 2


def ring_member(place):
    high = place // 2
    return 2 * high + (place % 2 + high) % 2


def flip(index, mask):
    bit = 1
    while bit <= mask:
        if mask & bit:
            index = index + bit * (1 - 2 * (index // bit % 2))
        bit *= 2
    return index


def bits(size):
    assert size & (size - 1) == 0
    return size.bit_length() - 1


def dot_rows(left, right):
    return lax.dot_general(
        left, right, (((1,), (1,)), ((), ())), preferred_element_type=jnp.float32
    )


def class_kernel(
    members,
    owners,
    sub,
    steps,
    labels_ref,
    places_ref,
    pick_ref,
    counts_ref,
    sketch_ref,
    gain_ref,
    cover_ref,
    sketch_part_ref,
    table_ref,
    out_ref,
    rows_ref,
    picks_ref,
    place_ref,
    inner_ref,
    pick_inner_ref,
    squares_ref,
    pick_squares_ref,
    bound_ref,
    wide_ref,
    row_gain_ref,
    gains_ref,
    final_ref,
    s_sem,
    a_send,
    a_recv,
    b_send,
    b_recv,
    x_send,
    x_recv,
    p_send,
    p_recv,
    m_send,
    m_recv,
    g_send,
    g_recv,
):
    member = lax.axis_index("dp")
    owner = lax.axis_index("cls")
    row_count, width = sketch_ref.shape
    parts, part = out_ref.shape[0], out_ref.shape[-1]
    chunks = rows_ref.shape[2]
    lanes = owners * UNIT
    capacity = chunks * lanes
    half = members // 2
    slots = half + 1
    pairs = owners // 2
    window = min(WINDOW, parts - 1)
    place = ring_place(member)
    step = 1 - 2 * (owner % 2)
    ring = (step * place + members) % members
    cut_chunk = chunks // 2
    gets_first = ring < half
    gets_second = (ring >= 1) & (ring <= half)
    gives_first = (ring + 1) % members < half
    gives_second = ring >= half
    scale = 1.0 / width
    order = [*range(pairs // 2, pairs), *range(pairs // 2 - 1, -1, -1)]

    barrier = pltpu.get_barrier_semaphore()
    for mask in range(1, owners):
        pl.semaphore_signal(
            barrier, inc=1, device_id=(member, flip(owner, mask)), device_id_type=MESH
        )
    for hop in range(1, members):
        pl.semaphore_signal(
            barrier,
            inc=1,
            device_id=(ring_member((place + hop) % members), owner),
            device_id_type=MESH,
        )

    def fetch(f):
        low = pl.multiple_of(f * part, part)
        return pltpu.make_async_copy(
            sketch_ref.at[:, pl.ds(low, part)], sketch_part_ref.at[f], s_sem.at[f]
        )

    def dispatch(f, mask):
        target = flip(owner, mask)
        return pltpu.make_async_remote_copy(
            src_ref=out_ref.at[f, target],
            dst_ref=rows_ref.at[0, f, :, owner],
            send_sem=a_send.at[f, mask - 1],
            recv_sem=a_recv.at[f, mask - 1],
            device_id=(member, target),
            device_id_type=MESH,
        )

    def dispatch_all(f):
        for pair in order:
            for mask in (2 * pair, 2 * pair + 1):
                if mask:
                    dispatch(f, mask).start()

    def sources(pair):
        return pl.ds(2 * flip(owner // 2, pair), 2)

    def share(f, hop, pair):
        target = ring_member((place + step * hop + members) % members)
        return pltpu.make_async_remote_copy(
            src_ref=rows_ref.at[0, f, :, sources(pair)],
            dst_ref=rows_ref.at[hop, f, :, sources(pair)],
            send_sem=b_send.at[f, hop - 1, pair],
            recv_sem=b_recv.at[f, hop - 1, pair],
            device_id=(target, owner),
            device_id_type=MESH,
        )

    def share_first(f, pair):
        return pltpu.make_async_remote_copy(
            src_ref=rows_ref.at[half - 1, f, :cut_chunk, sources(pair)],
            dst_ref=rows_ref.at[half, f, :cut_chunk, sources(pair)],
            send_sem=x_send.at[f, 0, pair],
            recv_sem=x_recv.at[f, 0, pair],
            device_id=(ring_member((place + step + members) % members), owner),
            device_id_type=MESH,
        )

    def share_second(f, pair):
        target = ring_member((place + step * (half + 1) + members * half) % members)
        return pltpu.make_async_remote_copy(
            src_ref=rows_ref.at[0, f, cut_chunk:, sources(pair)],
            dst_ref=rows_ref.at[half, f, cut_chunk:, sources(pair)],
            send_sem=x_send.at[f, 1, pair],
            recv_sem=x_recv.at[f, 1, pair],
            device_id=(target, owner),
            device_id_type=MESH,
        )

    def share_picks(f, hop):
        return pltpu.make_async_remote_copy(
            src_ref=picks_ref.at[0, f],
            dst_ref=picks_ref.at[hop, f],
            send_sem=p_send.at[f, hop - 1],
            recv_sem=p_recv.at[f, hop - 1],
            device_id=(ring_member((place + hop) % members), owner),
            device_id_type=MESH,
        )

    def share_bound(hop):
        return pltpu.make_async_remote_copy(
            src_ref=bound_ref.at[0],
            dst_ref=bound_ref.at[hop],
            send_sem=m_send.at[hop - 1],
            recv_sem=m_recv.at[hop - 1],
            device_id=(ring_member((place + hop) % members), owner),
            device_id_type=MESH,
        )

    def share_gains(hop):
        target = ring_member((place + hop) % members)
        return pltpu.make_async_remote_copy(
            src_ref=gains_ref.at[target * sub // UNIT],
            dst_ref=final_ref.at[members - hop],
            send_sem=g_send.at[hop - 1],
            recv_sem=g_recv.at[hop - 1],
            device_id=(target, owner),
            device_id_type=MESH,
        )

    def prepare(f):
        fetch(f).wait()
        block = jnp.dot(
            table_ref[...],
            sketch_part_ref[f],
            preferred_element_type=jnp.float32,
        ).astype(out_ref.dtype)
        out_ref[f] = block.reshape(out_ref.shape[1:])
        rows_ref[0, f, :, owner] = out_ref[f, owner]

    def part_rows(slot, f):
        return rows_ref[slot, f].reshape(capacity, part)

    def multiply(slot, f, left=0, first=0, last=chunks):
        low, high = first * lanes, last * lanes
        block = rows_ref[slot, f, first:last].reshape(high - low, part)
        product = dot_rows(part_rows(left, f), block)
        for chunk in range(first, last):
            cut = slice(chunk * lanes - low, (chunk + 1) * lanes - low)
            inner_ref[slot * chunks + chunk] += product[:, cut]
        total = jnp.zeros((high - low, 128), jnp.float32)
        for spot in range(0, part, 128):
            wide = block[:, spot : spot + 128].astype(jnp.float32)
            total = total + wide * wide
        squares_ref[slot, low:high] += total

    def multiply_picks(slot, f, picks, first=0, last=chunks):
        low, high = first * lanes, last * lanes
        block = rows_ref[slot, f, first:last].reshape(high - low, part)
        pick_inner_ref[slot, :, low:high] += dot_rows(picks, block)

    def own_part(f):
        picks_ref[0, f] = lax.dot_general(
            pick_table,
            part_rows(0, f),
            (((1,), (0,)), ((), ())),
            preferred_element_type=jnp.float32,
        ).astype(picks_ref.dtype)
        multiply(0, f)
        for hop in range(1, members):
            share_picks(f, hop).start()

    def other_part(f):
        for pair in range(pairs):
            for hop in range(1, half):
                share(f, hop, pair).wait_recv()

            @pl.when(gives_first)
            def _(pair=pair):
                share_first(f, pair).start()

        for hop in range(1, members):
            share_picks(f, hop).wait_recv()
        picks = picks_ref[0, f].astype(jnp.float32)
        for hop in range(1, members):
            picks = picks + picks_ref[hop, f].astype(jnp.float32)
        total = jnp.zeros((PICK_ROWS, 128), jnp.float32)
        for low in range(0, part, 128):
            wide = picks[:, low : low + 128]
            total = total + wide * wide
        pick_squares_ref[...] += total
        picks = picks.astype(picks_ref.dtype)
        multiply_picks(0, f, picks)
        for hop in range(1, half):
            multiply(hop, f)
            multiply_picks(hop, f, picks)

        @pl.when(gets_second)
        def _():
            for pair in range(pairs):
                share_second(f, pair).wait_recv()
            multiply(half, f, 1, cut_chunk, chunks)
            multiply_picks(half, f, picks, cut_chunk, chunks)

        @pl.when(gets_first)
        def _():
            for pair in range(pairs):
                share_first(f, pair).wait_recv()
            multiply(half, f, 0, 0, cut_chunk)
            multiply_picks(half, f, picks, 0, cut_chunk)

    for f in range(parts):
        fetch(f).start()
    label_bits, place_bits, sub_bits = bits(members), bits(members * owners * sub), bits(sub)
    unit_bits = bits(UNIT)
    places = places_ref[...]
    target = (labels_ref[...] << label_bits) + (places >> place_bits)
    target = (target << sub_bits) + (places & (sub - 1))
    table_ref[...] = (
        lax.broadcasted_iota(jnp.int32, (2 * row_count, row_count), 0) == target
    ).astype(table_ref.dtype)
    for f in range(window + 1):
        prepare(f)
    pl.semaphore_wait(barrier, owners + members - 2)
    for f in range(window):
        dispatch_all(f)

    inner_ref[...] = jnp.zeros_like(inner_ref)
    pick_inner_ref[...] = jnp.zeros_like(pick_inner_ref)
    squares_ref[...] = jnp.zeros_like(squares_ref)
    pick_squares_ref[...] = jnp.zeros_like(pick_squares_ref)
    row_gain_ref[...] = jnp.zeros_like(row_gain_ref)

    chosen = pick_ref[...]
    source = (chosen & (members * owners * sub - 1)) >> sub_bits
    offset = ((chosen >> place_bits) << sub_bits) + (chosen & (sub - 1))
    chosen = ((offset >> unit_bits) << bits(owners)) + (source & (owners - 1))
    chosen = (chosen << unit_bits) + (offset & (UNIT - 1)) + (source >> bits(owners)) * capacity
    turn_row = lax.broadcasted_iota(jnp.int32, (PICK_ROWS, capacity), 0)
    wanted = jnp.full((PICK_ROWS, capacity), -1, jnp.int32)
    for turn in range(steps):
        wanted = jnp.where(turn_row == turn, chosen[:, turn : turn + 1], wanted)
    pick_table = (
        lax.broadcasted_iota(jnp.int32, (PICK_ROWS, capacity), 1) + member * capacity == wanted
    ).astype(rows_ref.dtype)

    lows = UNIT // sub
    lane = lax.broadcasted_iota(jnp.int32, (members * owners, lanes), 1)
    source = lax.broadcasted_iota(jnp.int32, (members * owners, lanes), 0)
    spot = lax.broadcasted_iota(jnp.int32, (1, lanes), 1) & (sub - 1)
    for ahead in range(members):
        block = ring_member((place + ahead) % members)
        filled = jnp.zeros((chunks, lanes), jnp.float32)
        for low in range(lows):
            spread_out = (source == block * owners + (lane >> unit_bits)) & (
                ((lane >> sub_bits) & (lows - 1)) == low
            )
            filled = filled + jnp.dot(
                counts_ref[low].astype(jnp.float32).astype(jnp.bfloat16),
                spread_out.astype(jnp.bfloat16),
                preferred_element_type=jnp.float32,
            )
        place_ref[ahead] = (filled > spot.astype(jnp.float32)).astype(jnp.float32)
    total = jnp.sum(counts_ref[...].astype(jnp.float32), axis=0)
    total = jnp.sum(jnp.sum(total, axis=0, keepdims=True), axis=1, keepdims=True)

    @pl.loop(0, parts)
    def _(f):
        for pair in range(pairs):
            for mask in (2 * pair, 2 * pair + 1):
                if mask:
                    dispatch(f, mask).wait_recv()
            for hop in range(1, half):
                share(f, hop, pair).start()

            @pl.when(gives_second)
            def _(pair=pair):
                share_second(f, pair).start()

        @pl.when(f + window < parts)
        def _():
            dispatch_all(f + window)

        @pl.when(f + window + 1 < parts)
        def _():
            prepare(f + window + 1)

        own_part(f)

        @pl.when(f > 0)
        def _():
            other_part(f - 1)

    other_part(parts - 1)

    def block_row(behind):
        rows = place_ref[(members * half - step * behind) % members]
        return jnp.concatenate([rows[chunk : chunk + 1] for chunk in range(chunks)], axis=1)

    def valid_row(slot):
        if slot < half:
            return block_row(slot)
        split = cut_chunk * lanes
        first = jnp.where(gets_first, block_row(half)[:, :split], 0.0)
        second = jnp.where(gets_second, block_row(half + 1)[:, split:], 0.0)
        return jnp.concatenate([first, second], axis=1)

    def turned(row):
        return jnp.transpose(jnp.broadcast_to(row, (128, capacity)))

    valid = [valid_row(slot) > 0.5 for slot in range(slots)]
    norm = [
        jnp.sum(jnp.transpose(squares_ref[slot]), axis=0, keepdims=True) * scale
        for slot in range(slots)
    ]
    pick_norm = jnp.sum(pick_squares_ref[...], axis=1, keepdims=True) * scale

    def repeat(block):
        if lanes > 128:
            block = jnp.concatenate([block] * (lanes // 128), axis=1)
        return block

    def left_of(slot, chunk):
        return 1 if slot == half and chunk >= cut_chunk else 0

    for left in range(2):
        wide_ref[left, 0] = turned(jnp.where(valid[left], norm[left], -FAR))
    largest = jnp.zeros((1, lanes), jnp.float32)
    for slot in range(slots):
        for chunk in range(chunks):
            cut = slice(chunk * lanes, (chunk + 1) * lanes)
            near = repeat(wide_ref[left_of(slot, chunk), 0])
            tile = jnp.max(
                near - (2.0 * scale) * inner_ref[slot * chunks + chunk], axis=0, keepdims=True
            )
            tile = jnp.where(valid[slot][:, cut], tile + norm[slot][:, cut], 0.0)
            largest = jnp.maximum(largest, tile)
    largest = jnp.max(largest, axis=1, keepdims=True)
    bound_ref[0] = jnp.broadcast_to(largest, bound_ref.shape[1:])
    for hop in range(1, members):
        share_bound(hop).start()

    tops = []
    for slot in range(slots):
        top = None
        held = [jnp.broadcast_to(largest, (1, capacity))]
        for turn in range(steps):
            apart = (
                pick_norm[turn : turn + 1]
                + norm[slot]
                - (2.0 * scale) * pick_inner_ref[slot][turn : turn + 1]
            )
            top = apart if top is None else jnp.minimum(top, apart)
            held.append(top)
        tops.append(held)

    for left in range(2):
        for turn in range(steps):
            wide_ref[left, turn] = turned(
                jnp.where(valid[left], tops[left][turn] - norm[left], -FAR)
            )
        wide_ref[left, steps] = turned(-norm[left])
    sizes = [
        jnp.sum(valid[left].astype(jnp.float32), axis=1, keepdims=True) for left in range(2)
    ]
    far_sizes = [jnp.zeros((1, 1), jnp.float32) for left in range(2)]

    for slot in range(slots):
        for chunk in range(chunks):
            cut = slice(chunk * lanes, (chunk + 1) * lanes)
            tile = (2.0 * scale) * inner_ref[slot * chunks + chunk] - norm[slot][:, cut]
            gained = []
            left = left_of(slot, chunk)
            for turn in range(steps):
                gained.append(
                    jnp.sum(
                        jnp.maximum(tile + repeat(wide_ref[left, turn]), 0.0),
                        axis=0,
                        keepdims=True,
                    )
                )
                if slot > 0:
                    far = jnp.where(valid[slot][:, cut], tops[slot][turn][:, cut], -FAR)
                    each = jnp.maximum(tile + repeat(wide_ref[left, steps]) + far, 0.0)
                    for low in range(0, lanes, 128):
                        row_gain_ref[left, turn] += each[:, low : low + 128]
            gained.append(
                tops[0][steps][:, cut] if slot == 0 else jnp.zeros((1, lanes), jnp.float32)
            )
            gained.append(jnp.broadcast_to(largest * sizes[left], (1, lanes)))
            if slot == half:
                gets = gets_second if left else gets_first
                gained = [jnp.where(gets, row, 0.0) for row in gained]
            if slot > 0:
                far_sizes[left] = far_sizes[left] + jnp.sum(
                    valid[slot][:, cut].astype(jnp.float32), axis=1, keepdims=True
                )
            gained.append(jnp.zeros((8 - steps - 2, lanes), jnp.float32))
            gains_ref[chunk, slot] = jnp.concatenate(gained, axis=0)
    for left in range(2):
        for turn in range(steps):
            row = jnp.sum(jnp.transpose(row_gain_ref[left, turn]), axis=0, keepdims=True)
            for chunk in range(chunks):
                cut = slice(chunk * lanes, (chunk + 1) * lanes)
                gains_ref[chunk, left, turn : turn + 1] += row[:, cut]
        for chunk in range(chunks):
            gains_ref[chunk, left, steps + 1 : steps + 2] += jnp.broadcast_to(
                largest * far_sizes[left], (1, lanes)
            )

    for hop in range(1, members):
        share_gains(hop).start()
    final_ref[0] = gains_ref[member * sub // UNIT]
    for hop in range(1, members):
        share_bound(hop).wait_recv()
    bound = bound_ref[0]
    for hop in range(1, members):
        bound = jnp.maximum(bound, bound_ref[hop])
    bound = bound[:1, :1]
    for hop in range(1, members):
        share_gains(hop).wait_recv()
    chunk_here = member * sub // UNIT
    second = chunk_here // cut_chunk
    for ahead in range(members):
        summed = final_ref[ahead, 0]
        for slot in range(1, slots):
            behind = slot if slot < half else half + second
            holder = (ahead + step * behind + members * half) % members
            summed = summed + final_ref[holder, slot]
        block = ring_member((place + ahead) % members)
        here = pl.ds(pl.multiple_of(block * lanes, lanes), lanes)
        used = place_ref[ahead, pl.ds(chunk_here, 1)]
        for turn in range(steps):
            row = summed[turn : turn + 1]
            if turn == 0:
                row = row + (total * bound - summed[steps + 1 : steps + 2])
            gain_ref[turn, :, here] = row * used / total
        cover_ref[:, here] = jnp.maximum(bound - summed[steps : steps + 1], 0.0) * used

    @pl.loop(0, parts)
    def _(f):
        for mask in range(1, owners):
            dispatch(f, mask).wait_send()
        for pair in range(pairs):
            for hop in range(1, half):
                share(f, hop, pair).wait_send()
        for hop in range(1, members):
            share_picks(f, hop).wait_send()

        @pl.when(gives_second)
        def _():
            for pair in range(pairs):
                share_second(f, pair).wait_send()

        @pl.when(gives_first)
        def _():
            for pair in range(pairs):
                share_first(f, pair).wait_send()

    for hop in range(1, members):
        share_bound(hop).wait_send()
        share_gains(hop).wait_send()


def class_gains(labels, places, picks, counts, sketches, members, owners, sub, steps):
    row_count, width = sketches.shape
    chunks = members * sub // UNIT
    lanes = owners * UNIT
    capacity = chunks * lanes
    slots = members // 2 + 1
    part = width // PARTS
    kind = sketches.dtype
    vmem = pl.BlockSpec(memory_space=pltpu.VMEM)
    dma = pltpu.SemaphoreType.DMA
    return pl.pallas_call(
        functools.partial(class_kernel, members, owners, sub, steps),
        out_shape=(
            jax.ShapeDtypeStruct((steps, 1, members * lanes), jnp.float32),
            jax.ShapeDtypeStruct((1, members * lanes), jnp.float32),
        ),
        in_specs=[vmem, vmem, vmem, vmem, pl.BlockSpec(memory_space=pl.ANY)],
        out_specs=(vmem, vmem),
        scratch_shapes=[
            pltpu.VMEM((PARTS, row_count, part), kind),
            pltpu.VMEM((2 * row_count, row_count), kind),
            pltpu.VMEM((PARTS, owners, chunks, UNIT, part), kind),
            pltpu.VMEM((slots, PARTS, chunks, owners, UNIT, part), kind),
            pltpu.VMEM((members, PARTS, PICK_ROWS, part), kind),
            pltpu.VMEM((members, chunks, lanes), jnp.float32),
            pltpu.VMEM((slots * chunks, capacity, lanes), jnp.float32),
            pltpu.VMEM((slots, PICK_ROWS, capacity), jnp.float32),
            pltpu.VMEM((slots, capacity, 128), jnp.float32),
            pltpu.VMEM((PICK_ROWS, 128), jnp.float32),
            pltpu.VMEM((members, 8, 128), jnp.float32),
            pltpu.VMEM((2, steps + 1, capacity, 128), jnp.float32),
            pltpu.VMEM((2, steps, capacity, 128), jnp.float32),
            pltpu.VMEM((chunks, slots, 8, lanes), jnp.float32),
            pltpu.VMEM((members, slots, 8, lanes), jnp.float32),
            dma((PARTS,)),
            dma((PARTS, owners - 1)),
            dma((PARTS, owners - 1)),
            dma((PARTS, members // 2 - 1, owners // 2)),
            dma((PARTS, members // 2 - 1, owners // 2)),
            dma((PARTS, 2, owners // 2)),
            dma((PARTS, 2, owners // 2)),
            dma((PARTS, members - 1)),
            dma((PARTS, members - 1)),
            dma((members - 1,)),
            dma((members - 1,)),
            dma((members - 1,)),
            dma((members - 1,)),
        ],
        compiler_params=pltpu.CompilerParams(
            collective_id=0, has_side_effects=True, vmem_limit_bytes=60 * 1024 * 1024
        ),
    )(labels, places, picks, counts, sketches)


def body(sketches, labels, places, counts, chosen):
    row_count = sketches.shape[0]
    members = lax.axis_size("dp")
    owners = lax.axis_size("cls")
    devices = members * owners
    sub = 2 * row_count // devices
    capacity = devices * sub
    chunks = members * sub // UNIT
    lows = UNIT // sub
    member = lax.axis_index("dp")
    steps = chosen.shape[0]

    filled = jnp.transpose(counts[0].reshape(chunks, lows, devices), (1, 0, 2))
    gain_scores, coverage = class_gains(
        labels.reshape(1, row_count),
        places.reshape(1, row_count),
        chosen.reshape(1, steps),
        filled,
        sketches,
        members,
        owners,
        sub,
        steps,
    )
    if lows > 1:
        gain_scores = lax.dynamic_index_in_dim(
            gain_scores.reshape(steps, 1, members * owners, lows, sub), member % lows, 3, False
        ).reshape(steps, 1, capacity)
        coverage = lax.dynamic_index_in_dim(
            coverage.reshape(1, members * owners, lows, sub), member % lows, 2, False
        ).reshape(1, capacity)
    return (gain_scores, coverage)


def solution(mesh):
    placed = (
        P(("dp", "cls"), None),
        P(("dp", "cls")),
        P(("dp", "cls")),
        P("cls", None, None),
        P(None, "cls"),
    )
    return jax.shard_map(
        body,
        mesh=mesh,
        in_specs=placed,
        out_specs=(P(None, "cls", "dp"), P("cls", "dp")),
        check_vma=False,
    )
```

```python
import functools

import jax
import jax.numpy as jnp
from jax import lax
from jax.experimental import pallas as pl
from jax.experimental.pallas import tpu as pltpu
from jax.sharding import PartitionSpec as P

MESH = pl.DeviceIdType.MESH
UNIT = 16
PICK_ROWS = 16
PARTS = 16
WINDOW = 2
FAR = 1e30


def ring_place(index):
    high = index // 2
    return 2 * high + (index % 2 + high) % 2


def ring_member(place):
    high = place // 2
    return 2 * high + (place % 2 + high) % 2


def flip(index, mask):
    bit = 1
    while bit <= mask:
        if mask & bit:
            index = index + bit * (1 - 2 * (index // bit % 2))
        bit *= 2
    return index


def bits(size):
    assert size & (size - 1) == 0
    return size.bit_length() - 1


def dot_rows(left, right):
    return lax.dot_general(
        left, right, (((1,), (1,)), ((), ())), preferred_element_type=jnp.float32
    )


def class_kernel(
    members,
    owners,
    sub,
    steps,
    labels_ref,
    places_ref,
    pick_ref,
    counts_ref,
    sketch_ref,
    gain_ref,
    cover_ref,
    sketch_part_ref,
    table_ref,
    out_ref,
    rows_ref,
    picks_ref,
    place_ref,
    inner_ref,
    pick_inner_ref,
    squares_ref,
    pick_squares_ref,
    bound_ref,
    wide_ref,
    row_gain_ref,
    gains_ref,
    final_ref,
    s_sem,
    a_send,
    a_recv,
    b_send,
    b_recv,
    x_send,
    x_recv,
    p_send,
    p_recv,
    m_send,
    m_recv,
    g_send,
    g_recv,
):
    member = lax.axis_index("dp")
    owner = lax.axis_index("cls")
    row_count, width = sketch_ref.shape
    parts, part = out_ref.shape[0], out_ref.shape[-1]
    chunks = rows_ref.shape[2]
    lanes = owners * UNIT
    capacity = chunks * lanes
    half = members // 2
    slots = half + 1
    pairs = owners // 2
    window = min(WINDOW, parts - 1)
    place = ring_place(member)
    step = 1 - 2 * (owner % 2)
    ring = (step * place + members) % members
    cut_chunk = chunks // 2
    gets_first = ring < half
    gets_second = (ring >= 1) & (ring <= half)
    gives_first = (ring + 1) % members < half
    gives_second = ring >= half
    scale = 1.0 / width

    barrier = pltpu.get_barrier_semaphore()
    for mask in range(1, owners):
        pl.semaphore_signal(
            barrier, inc=1, device_id=(member, flip(owner, mask)), device_id_type=MESH
        )
    for hop in range(1, members):
        pl.semaphore_signal(
            barrier,
            inc=1,
            device_id=(ring_member((place + hop) % members), owner),
            device_id_type=MESH,
        )

    def fetch(f):
        low = pl.multiple_of(f * part, part)
        return pltpu.make_async_copy(
            sketch_ref.at[:, pl.ds(low, part)], sketch_part_ref.at[f], s_sem.at[f]
        )

    def dispatch(f, mask):
        target = flip(owner, mask)
        return pltpu.make_async_remote_copy(
            src_ref=out_ref.at[f, target],
            dst_ref=rows_ref.at[0, f, :, owner],
            send_sem=a_send.at[f, mask - 1],
            recv_sem=a_recv.at[f, mask - 1],
            device_id=(member, target),
            device_id_type=MESH,
        )

    def dispatch_all(f):
        for pair in range(pairs - 1, -1, -1):
            for mask in (2 * pair, 2 * pair + 1):
                if mask:
                    dispatch(f, mask).start()

    def sources(pair):
        return pl.ds(2 * flip(owner // 2, pair), 2)

    def share(f, hop, pair):
        target = ring_member((place + step * hop + members) % members)
        return pltpu.make_async_remote_copy(
            src_ref=rows_ref.at[0, f, :, sources(pair)],
            dst_ref=rows_ref.at[hop, f, :, sources(pair)],
            send_sem=b_send.at[f, hop - 1, pair],
            recv_sem=b_recv.at[f, hop - 1, pair],
            device_id=(target, owner),
            device_id_type=MESH,
        )

    def share_first(f, pair):
        return pltpu.make_async_remote_copy(
            src_ref=rows_ref.at[half - 1, f, :cut_chunk, sources(pair)],
            dst_ref=rows_ref.at[half, f, :cut_chunk, sources(pair)],
            send_sem=x_send.at[f, 0, pair],
            recv_sem=x_recv.at[f, 0, pair],
            device_id=(ring_member((place + step + members) % members), owner),
            device_id_type=MESH,
        )

    def share_direct(f, pair):
        return pltpu.make_async_remote_copy(
            src_ref=rows_ref.at[0, f, :cut_chunk, sources(pair)],
            dst_ref=rows_ref.at[half, f, :cut_chunk, sources(pair)],
            send_sem=x_send.at[f, 0, pair],
            recv_sem=x_recv.at[f, 0, pair],
            device_id=(ring_member((place + half) % members), owner),
            device_id_type=MESH,
        )

    def share_second(f, pair):
        target = ring_member((place + step * (half + 1) + members * half) % members)
        return pltpu.make_async_remote_copy(
            src_ref=rows_ref.at[0, f, cut_chunk:, sources(pair)],
            dst_ref=rows_ref.at[half, f, cut_chunk:, sources(pair)],
            send_sem=x_send.at[f, 1, pair],
            recv_sem=x_recv.at[f, 1, pair],
            device_id=(target, owner),
            device_id_type=MESH,
        )

    def share_picks(f, hop):
        return pltpu.make_async_remote_copy(
            src_ref=picks_ref.at[0, f],
            dst_ref=picks_ref.at[hop, f],
            send_sem=p_send.at[f, hop - 1],
            recv_sem=p_recv.at[f, hop - 1],
            device_id=(ring_member((place + hop) % members), owner),
            device_id_type=MESH,
        )

    def share_bound(hop):
        return pltpu.make_async_remote_copy(
            src_ref=bound_ref.at[0],
            dst_ref=bound_ref.at[hop],
            send_sem=m_send.at[hop - 1],
            recv_sem=m_recv.at[hop - 1],
            device_id=(ring_member((place + hop) % members), owner),
            device_id_type=MESH,
        )

    def share_gains(hop):
        target = ring_member((place + hop) % members)
        return pltpu.make_async_remote_copy(
            src_ref=gains_ref.at[target * sub // UNIT],
            dst_ref=final_ref.at[members - hop],
            send_sem=g_send.at[hop - 1],
            recv_sem=g_recv.at[hop - 1],
            device_id=(target, owner),
            device_id_type=MESH,
        )

    def prepare(f):
        fetch(f).wait()
        block = jnp.dot(
            table_ref[...],
            sketch_part_ref[f],
            preferred_element_type=jnp.float32,
        ).astype(out_ref.dtype)
        out_ref[f] = block.reshape(out_ref.shape[1:])
        rows_ref[0, f, :, owner] = out_ref[f, owner]

    def part_rows(slot, f):
        return rows_ref[slot, f].reshape(capacity, part)

    def multiply(slot, f, left=0, first=0, last=chunks):
        low, high = first * lanes, last * lanes
        block = rows_ref[slot, f, first:last].reshape(high - low, part)
        product = dot_rows(part_rows(left, f), block)
        for chunk in range(first, last):
            cut = slice(chunk * lanes - low, (chunk + 1) * lanes - low)
            inner_ref[slot * chunks + chunk] += product[:, cut]
        total = jnp.zeros((high - low, 128), jnp.float32)
        for spot in range(0, part, 128):
            wide = block[:, spot : spot + 128].astype(jnp.float32)
            total = total + wide * wide
        squares_ref[slot, low:high] += total

    def multiply_picks(slot, f, picks, first=0, last=chunks):
        low, high = first * lanes, last * lanes
        block = rows_ref[slot, f, first:last].reshape(high - low, part)
        pick_inner_ref[slot, :, low:high] += dot_rows(picks, block)

    def own_part(f):
        picks_ref[0, f] = lax.dot_general(
            pick_table,
            part_rows(0, f),
            (((1,), (0,)), ((), ())),
            preferred_element_type=jnp.float32,
        ).astype(picks_ref.dtype)
        multiply(0, f)
        for hop in range(1, members):
            share_picks(f, hop).start()

    def other_part(f, forward=True):
        for pair in range(pairs):
            for hop in range(1, half):
                share(f, hop, pair).wait_recv()

            if forward:

                @pl.when(gives_first)
                def _(pair=pair):
                    share_first(f, pair).start()

        for hop in range(1, members):
            share_picks(f, hop).wait_recv()
        picks = picks_ref[0, f].astype(jnp.float32)
        for hop in range(1, members):
            picks = picks + picks_ref[hop, f].astype(jnp.float32)
        total = jnp.zeros((PICK_ROWS, 128), jnp.float32)
        for low in range(0, part, 128):
            wide = picks[:, low : low + 128]
            total = total + wide * wide
        pick_squares_ref[...] += total
        picks = picks.astype(picks_ref.dtype)
        multiply_picks(0, f, picks)
        for hop in range(1, half):
            multiply(hop, f)
            multiply_picks(hop, f, picks)

        @pl.when(gets_second)
        def _():
            for pair in range(pairs):
                share_second(f, pair).wait_recv()
            multiply(half, f, 1, cut_chunk, chunks)
            multiply_picks(half, f, picks, cut_chunk, chunks)

        @pl.when(gets_first)
        def _():
            for pair in range(pairs):
                share_first(f, pair).wait_recv()
            multiply(half, f, 0, 0, cut_chunk)
            multiply_picks(half, f, picks, 0, cut_chunk)

    for f in range(parts):
        fetch(f).start()
    label_bits, place_bits, sub_bits = bits(members), bits(members * owners * sub), bits(sub)
    unit_bits = bits(UNIT)
    places = places_ref[...]
    target = (labels_ref[...] << label_bits) + (places >> place_bits)
    target = (target << sub_bits) + (places & (sub - 1))
    table_ref[...] = (
        lax.broadcasted_iota(jnp.int32, (2 * row_count, row_count), 0) == target
    ).astype(table_ref.dtype)
    for f in range(window + 1):
        prepare(f)
    pl.semaphore_wait(barrier, owners + members - 2)
    for f in range(window):
        dispatch_all(f)

    inner_ref[...] = jnp.zeros_like(inner_ref)
    pick_inner_ref[...] = jnp.zeros_like(pick_inner_ref)
    squares_ref[...] = jnp.zeros_like(squares_ref)
    pick_squares_ref[...] = jnp.zeros_like(pick_squares_ref)
    row_gain_ref[...] = jnp.zeros_like(row_gain_ref)

    chosen = pick_ref[...]
    source = (chosen & (members * owners * sub - 1)) >> sub_bits
    offset = ((chosen >> place_bits) << sub_bits) + (chosen & (sub - 1))
    chosen = ((offset >> unit_bits) << bits(owners)) + (source & (owners - 1))
    chosen = (chosen << unit_bits) + (offset & (UNIT - 1)) + (source >> bits(owners)) * capacity
    turn_row = lax.broadcasted_iota(jnp.int32, (PICK_ROWS, capacity), 0)
    wanted = jnp.full((PICK_ROWS, capacity), -1, jnp.int32)
    for turn in range(steps):
        wanted = jnp.where(turn_row == turn, chosen[:, turn : turn + 1], wanted)
    pick_table = (
        lax.broadcasted_iota(jnp.int32, (PICK_ROWS, capacity), 1) + member * capacity == wanted
    ).astype(rows_ref.dtype)

    lows = UNIT // sub
    lane = lax.broadcasted_iota(jnp.int32, (members * owners, lanes), 1)
    source = lax.broadcasted_iota(jnp.int32, (members * owners, lanes), 0)
    spot = lax.broadcasted_iota(jnp.int32, (1, lanes), 1) & (sub - 1)
    for ahead in range(members):
        block = ring_member((place + ahead) % members)
        filled = jnp.zeros((chunks, lanes), jnp.float32)
        for low in range(lows):
            spread_out = (source == block * owners + (lane >> unit_bits)) & (
                ((lane >> sub_bits) & (lows - 1)) == low
            )
            filled = filled + jnp.dot(
                counts_ref[low].astype(jnp.float32).astype(jnp.bfloat16),
                spread_out.astype(jnp.bfloat16),
                preferred_element_type=jnp.float32,
            )
        place_ref[ahead] = (filled > spot.astype(jnp.float32)).astype(jnp.float32)
    total = jnp.sum(counts_ref[...].astype(jnp.float32), axis=0)
    total = jnp.sum(jnp.sum(total, axis=0, keepdims=True), axis=1, keepdims=True)

    @pl.loop(0, parts)
    def _(f):
        for pair in range(pairs):
            for mask in (2 * pair, 2 * pair + 1):
                if mask:
                    dispatch(f, mask).wait_recv()
            for hop in range(1, half):
                share(f, hop, pair).start()

            @pl.when(gives_second)
            def _(pair=pair):
                share_second(f, pair).start()

            @pl.when(gives_second & (f == parts - 1))
            def _(pair=pair):
                share_direct(f, pair).start()

        @pl.when(f + window < parts)
        def _():
            dispatch_all(f + window)

        @pl.when(f + window + 1 < parts)
        def _():
            prepare(f + window + 1)

        own_part(f)

        @pl.when(f > 0)
        def _():
            other_part(f - 1)

    other_part(parts - 1, forward=False)

    def block_row(behind):
        rows = place_ref[(members * half - step * behind) % members]
        return jnp.concatenate([rows[chunk : chunk + 1] for chunk in range(chunks)], axis=1)

    def valid_row(slot):
        if slot < half:
            return block_row(slot)
        split = cut_chunk * lanes
        first = jnp.where(gets_first, block_row(half)[:, :split], 0.0)
        second = jnp.where(gets_second, block_row(half + 1)[:, split:], 0.0)
        return jnp.concatenate([first, second], axis=1)

    def turned(row):
        return jnp.transpose(jnp.broadcast_to(row, (128, capacity)))

    valid = [valid_row(slot) > 0.5 for slot in range(slots)]
    norm = [
        jnp.sum(jnp.transpose(squares_ref[slot]), axis=0, keepdims=True) * scale
        for slot in range(slots)
    ]
    pick_norm = jnp.sum(pick_squares_ref[...], axis=1, keepdims=True) * scale

    def repeat(block):
        if lanes > 128:
            block = jnp.concatenate([block] * (lanes // 128), axis=1)
        return block

    def left_of(slot, chunk):
        return 1 if slot == half and chunk >= cut_chunk else 0

    tops = []
    for slot in range(slots):
        held = []
        for turn in range(steps):
            apart = (
                pick_norm[turn : turn + 1]
                + norm[slot]
                - (2.0 * scale) * pick_inner_ref[slot][turn : turn + 1]
            )
            held.append(jnp.minimum(held[-1], apart) if held else apart)
        tops.append(held)

    for left in range(2):
        closed = turned(jnp.where(valid[left], -norm[left], -FAR))
        wide_ref[left, steps] = closed
        wide_ref[left, 0] = jnp.where(closed > -0.5 * FAR, -closed, -FAR)
        for turn in range(1, steps):
            wide_ref[left, turn] = turned(
                jnp.where(valid[left], tops[left][turn - 1] - norm[left], -FAR)
            )

    largest = jnp.zeros((1, lanes), jnp.float32)
    for slot in range(slots):
        for chunk in range(chunks):
            cut = slice(chunk * lanes, (chunk + 1) * lanes)
            near = repeat(wide_ref[left_of(slot, chunk), 0])
            there = jnp.where(valid[slot][:, cut], norm[slot][:, cut], FAR)
            tile = (2.0 * scale) * inner_ref[slot * chunks + chunk] - there
            inner_ref[slot * chunks + chunk] = tile
            tile = jnp.max(near - tile, axis=0, keepdims=True)
            largest = jnp.maximum(largest, jnp.where(valid[slot][:, cut], tile, 0.0))
    largest = jnp.max(largest, axis=1, keepdims=True)
    bound_ref[0] = jnp.broadcast_to(largest, bound_ref.shape[1:])
    for hop in range(1, members):
        share_bound(hop).start()
    for left in range(2):
        wide_ref[left, 0] = wide_ref[left, steps] + largest

    sizes = [
        jnp.sum(valid[left].astype(jnp.float32), axis=1, keepdims=True) for left in range(2)
    ]
    far_sizes = [jnp.zeros((1, 1), jnp.float32) for left in range(2)]

    for slot in range(slots):
        for chunk in range(chunks):
            cut = slice(chunk * lanes, (chunk + 1) * lanes)
            tile = inner_ref[slot * chunks + chunk]
            gained = []
            left = left_of(slot, chunk)
            if slot > 0:
                closed = tile + repeat(wide_ref[left, steps])
            for turn in range(steps):
                each = jnp.maximum(tile + repeat(wide_ref[left, turn]), 0.0)
                gained.append(jnp.sum(each, axis=0, keepdims=True))
                if slot > 0:
                    if turn > 0:
                        each = jnp.maximum(closed + tops[slot][turn - 1][:, cut], 0.0)
                    for low in range(0, lanes, 128):
                        row_gain_ref[left, turn] += each[:, low : low + 128]
            gained.append(
                tops[0][steps - 1][:, cut] if slot == 0 else jnp.zeros((1, lanes), jnp.float32)
            )
            gained.append(jnp.broadcast_to(largest * sizes[left], (1, lanes)))
            if slot == half:
                gets = gets_second if left else gets_first
                gained = [jnp.where(gets, row, 0.0) for row in gained]
            if slot > 0:
                far_sizes[left] = far_sizes[left] + jnp.sum(
                    valid[slot][:, cut].astype(jnp.float32), axis=1, keepdims=True
                )
            gained.append(jnp.zeros((8 - steps - 2, lanes), jnp.float32))
            gains_ref[chunk, slot] = jnp.concatenate(gained, axis=0)
    for left in range(2):
        for turn in range(steps):
            row = jnp.sum(jnp.transpose(row_gain_ref[left, turn]), axis=0, keepdims=True)
            for chunk in range(chunks):
                cut = slice(chunk * lanes, (chunk + 1) * lanes)
                gains_ref[chunk, left, turn : turn + 1] += row[:, cut]
        for chunk in range(chunks):
            gains_ref[chunk, left, steps + 1 : steps + 2] += jnp.broadcast_to(
                largest * far_sizes[left], (1, lanes)
            )

    for hop in range(1, members):
        share_gains(hop).start()
    final_ref[0] = gains_ref[member * sub // UNIT]

    @pl.loop(0, parts)
    def _(f):
        for mask in range(1, owners):
            dispatch(f, mask).wait_send()
        for pair in range(pairs):
            for hop in range(1, half):
                share(f, hop, pair).wait_send()
        for hop in range(1, members):
            share_picks(f, hop).wait_send()

        @pl.when(gives_second)
        def _():
            for pair in range(pairs):
                share_second(f, pair).wait_send()

        @pl.when(gives_second & (f == parts - 1))
        def _():
            for pair in range(pairs):
                share_direct(f, pair).wait_send()

        @pl.when(gives_first & (f < parts - 1))
        def _():
            for pair in range(pairs):
                share_first(f, pair).wait_send()

    for hop in range(1, members):
        share_bound(hop).wait_recv()
    bound = bound_ref[0]
    for hop in range(1, members):
        bound = jnp.maximum(bound, bound_ref[hop])
    bound = bound[:1, :1]
    for hop in range(1, members):
        share_gains(hop).wait_recv()
    chunk_here = member * sub // UNIT
    second = chunk_here // cut_chunk
    for ahead in range(members):
        summed = final_ref[ahead, 0]
        for slot in range(1, slots):
            behind = slot if slot < half else half + second
            holder = (ahead + step * behind + members * half) % members
            summed = summed + final_ref[holder, slot]
        block = ring_member((place + ahead) % members)
        here = pl.ds(pl.multiple_of(block * lanes, lanes), lanes)
        used = place_ref[ahead, pl.ds(chunk_here, 1)]
        for turn in range(steps):
            row = summed[turn : turn + 1]
            if turn == 0:
                row = row + (total * bound - summed[steps + 1 : steps + 2])
            gain_ref[turn, :, here] = row * used / total
        cover_ref[:, here] = jnp.maximum(bound - summed[steps : steps + 1], 0.0) * used

    for hop in range(1, members):
        share_bound(hop).wait_send()
        share_gains(hop).wait_send()


def class_gains(labels, places, picks, counts, sketches, members, owners, sub, steps):
    row_count, width = sketches.shape
    chunks = members * sub // UNIT
    lanes = owners * UNIT
    capacity = chunks * lanes
    slots = members // 2 + 1
    part = width // PARTS
    kind = sketches.dtype
    vmem = pl.BlockSpec(memory_space=pltpu.VMEM)
    dma = pltpu.SemaphoreType.DMA
    return pl.pallas_call(
        functools.partial(class_kernel, members, owners, sub, steps),
        out_shape=(
            jax.ShapeDtypeStruct((steps, 1, members * lanes), jnp.float32),
            jax.ShapeDtypeStruct((1, members * lanes), jnp.float32),
        ),
        in_specs=[vmem, vmem, vmem, vmem, pl.BlockSpec(memory_space=pl.ANY)],
        out_specs=(vmem, vmem),
        scratch_shapes=[
            pltpu.VMEM((PARTS, row_count, part), kind),
            pltpu.VMEM((2 * row_count, row_count), kind),
            pltpu.VMEM((PARTS, owners, chunks, UNIT, part), kind),
            pltpu.VMEM((slots, PARTS, chunks, owners, UNIT, part), kind),
            pltpu.VMEM((members, PARTS, PICK_ROWS, part), kind),
            pltpu.VMEM((members, chunks, lanes), jnp.float32),
            pltpu.VMEM((slots * chunks, capacity, lanes), jnp.float32),
            pltpu.VMEM((slots, PICK_ROWS, capacity), jnp.float32),
            pltpu.VMEM((slots, capacity, 128), jnp.float32),
            pltpu.VMEM((PICK_ROWS, 128), jnp.float32),
            pltpu.VMEM((members, 8, 128), jnp.float32),
            pltpu.VMEM((2, steps + 1, capacity, 128), jnp.float32),
            pltpu.VMEM((2, steps, capacity, 128), jnp.float32),
            pltpu.VMEM((chunks, slots, 8, lanes), jnp.float32),
            pltpu.VMEM((members, slots, 8, lanes), jnp.float32),
            dma((PARTS,)),
            dma((PARTS, owners - 1)),
            dma((PARTS, owners - 1)),
            dma((PARTS, members // 2 - 1, owners // 2)),
            dma((PARTS, members // 2 - 1, owners // 2)),
            dma((PARTS, 2, owners // 2)),
            dma((PARTS, 2, owners // 2)),
            dma((PARTS, members - 1)),
            dma((PARTS, members - 1)),
            dma((members - 1,)),
            dma((members - 1,)),
            dma((members - 1,)),
            dma((members - 1,)),
        ],
        compiler_params=pltpu.CompilerParams(
            collective_id=0, has_side_effects=True, vmem_limit_bytes=60 * 1024 * 1024
        ),
    )(labels, places, picks, counts, sketches)


def body(sketches, labels, places, counts, chosen):
    row_count = sketches.shape[0]
    members = lax.axis_size("dp")
    owners = lax.axis_size("cls")
    devices = members * owners
    sub = 2 * row_count // devices
    capacity = devices * sub
    chunks = members * sub // UNIT
    lows = UNIT // sub
    member = lax.axis_index("dp")
    steps = chosen.shape[0]

    filled = jnp.transpose(counts[0].reshape(chunks, lows, devices), (1, 0, 2))
    gain_scores, coverage = class_gains(
        labels.reshape(1, row_count),
        places.reshape(1, row_count),
        chosen.reshape(1, steps),
        filled,
        sketches,
        members,
        owners,
        sub,
        steps,
    )
    if lows > 1:
        gain_scores = lax.dynamic_index_in_dim(
            gain_scores.reshape(steps, 1, members * owners, lows, sub), member % lows, 3, False
        ).reshape(steps, 1, capacity)
        coverage = lax.dynamic_index_in_dim(
            coverage.reshape(1, members * owners, lows, sub), member % lows, 2, False
        ).reshape(1, capacity)
    return (gain_scores, coverage)


def solution(mesh):
    placed = (
        P(("dp", "cls"), None),
        P(("dp", "cls")),
        P(("dp", "cls")),
        P("cls", None, None),
        P(None, "cls"),
    )
    return jax.shard_map(
        body,
        mesh=mesh,
        in_specs=placed,
        out_specs=(P(None, "cls", "dp"), P("cls", "dp")),
        check_vma=False,
    )
```

```python
import functools

import jax
import jax.numpy as jnp
from jax import lax
from jax.experimental import pallas as pl
from jax.experimental.pallas import tpu as pltpu
from jax.sharding import PartitionSpec as P

MESH = pl.DeviceIdType.MESH
UNIT = 16
PICK_ROWS = 16
PARTS = 16
WINDOW = 2
FAR = 1e30


def ring_place(index):
    high = index // 2
    return 2 * high + (index % 2 + high) % 2


def ring_member(place):
    high = place // 2
    return 2 * high + (place % 2 + high) % 2


def flip(index, mask):
    bit = 1
    while bit <= mask:
        if mask & bit:
            index = index + bit * (1 - 2 * (index // bit % 2))
        bit *= 2
    return index


def bits(size):
    assert size & (size - 1) == 0
    return size.bit_length() - 1


def dot_rows(left, right):
    return lax.dot_general(
        left, right, (((1,), (1,)), ((), ())), preferred_element_type=jnp.float32
    )


def class_kernel(
    members,
    owners,
    sub,
    steps,
    labels_ref,
    places_ref,
    pick_ref,
    counts_ref,
    sketch_ref,
    gain_ref,
    cover_ref,
    sketch_part_ref,
    table_ref,
    out_ref,
    rows_ref,
    picks_ref,
    place_ref,
    inner_ref,
    pick_inner_ref,
    squares_ref,
    pick_squares_ref,
    bound_ref,
    wide_ref,
    row_gain_ref,
    gains_ref,
    final_ref,
    s_sem,
    a_send,
    a_recv,
    b_send,
    b_recv,
    x_send,
    x_recv,
    p_send,
    p_recv,
    m_send,
    m_recv,
    g_send,
    g_recv,
):
    member = lax.axis_index("dp")
    owner = lax.axis_index("cls")
    row_count, width = sketch_ref.shape
    parts, part = out_ref.shape[0], out_ref.shape[-1]
    chunks = rows_ref.shape[2]
    lanes = owners * UNIT
    capacity = chunks * lanes
    half = members // 2
    slots = half + 1
    pairs = owners // 2
    window = min(WINDOW, parts - 1)
    place = ring_place(member)
    step = 1 - 2 * (owner % 2)
    ring = (step * place + members) % members
    cut_chunk = chunks // 2
    gets_first = ring < half
    gets_second = (ring >= 1) & (ring <= half)
    gives_first = (ring + 1) % members < half
    gives_second = ring >= half
    scale = 1.0 / width

    barrier = pltpu.get_barrier_semaphore()
    for mask in range(1, owners):
        pl.semaphore_signal(
            barrier, inc=1, device_id=(member, flip(owner, mask)), device_id_type=MESH
        )
    for hop in range(1, members):
        pl.semaphore_signal(
            barrier,
            inc=1,
            device_id=(ring_member((place + hop) % members), owner),
            device_id_type=MESH,
        )

    def fetch(f):
        low = pl.multiple_of(f * part, part)
        return pltpu.make_async_copy(
            sketch_ref.at[:, pl.ds(low, part)], sketch_part_ref.at[f], s_sem.at[f]
        )

    def dispatch(f, mask):
        target = flip(owner, mask)
        return pltpu.make_async_remote_copy(
            src_ref=out_ref.at[f, target],
            dst_ref=rows_ref.at[0, f, :, owner],
            send_sem=a_send.at[f, mask - 1],
            recv_sem=a_recv.at[f, mask - 1],
            device_id=(member, target),
            device_id_type=MESH,
        )

    def dispatch_all(f):
        for pair in range(pairs - 1, -1, -1):
            for mask in (2 * pair, 2 * pair + 1):
                if mask:
                    dispatch(f, mask).start()

    def sources(pair):
        return pl.ds(2 * flip(owner // 2, pair), 2)

    def share(f, hop, pair):
        target = ring_member((place + step * hop + members) % members)
        return pltpu.make_async_remote_copy(
            src_ref=rows_ref.at[0, f, :, sources(pair)],
            dst_ref=rows_ref.at[hop, f, :, sources(pair)],
            send_sem=b_send.at[f, hop - 1, pair],
            recv_sem=b_recv.at[f, hop - 1, pair],
            device_id=(target, owner),
            device_id_type=MESH,
        )

    def share_first(f, pair):
        return pltpu.make_async_remote_copy(
            src_ref=rows_ref.at[half - 1, f, :cut_chunk, sources(pair)],
            dst_ref=rows_ref.at[half, f, :cut_chunk, sources(pair)],
            send_sem=x_send.at[f, 0, pair],
            recv_sem=x_recv.at[f, 0, pair],
            device_id=(ring_member((place + step + members) % members), owner),
            device_id_type=MESH,
        )

    def share_direct(f, pair):
        return pltpu.make_async_remote_copy(
            src_ref=rows_ref.at[0, f, :cut_chunk, sources(pair)],
            dst_ref=rows_ref.at[half, f, :cut_chunk, sources(pair)],
            send_sem=x_send.at[f, 0, pair],
            recv_sem=x_recv.at[f, 0, pair],
            device_id=(ring_member((place + half) % members), owner),
            device_id_type=MESH,
        )

    def share_second(f, pair):
        target = ring_member((place + step * (half + 1) + members * half) % members)
        return pltpu.make_async_remote_copy(
            src_ref=rows_ref.at[0, f, cut_chunk:, sources(pair)],
            dst_ref=rows_ref.at[half, f, cut_chunk:, sources(pair)],
            send_sem=x_send.at[f, 1, pair],
            recv_sem=x_recv.at[f, 1, pair],
            device_id=(target, owner),
            device_id_type=MESH,
        )

    def share_picks(f, hop):
        return pltpu.make_async_remote_copy(
            src_ref=picks_ref.at[0, f],
            dst_ref=picks_ref.at[hop, f],
            send_sem=p_send.at[f, hop - 1],
            recv_sem=p_recv.at[f, hop - 1],
            device_id=(ring_member((place + hop) % members), owner),
            device_id_type=MESH,
        )

    def share_bound(hop):
        return pltpu.make_async_remote_copy(
            src_ref=bound_ref.at[0],
            dst_ref=bound_ref.at[hop],
            send_sem=m_send.at[hop - 1],
            recv_sem=m_recv.at[hop - 1],
            device_id=(ring_member((place + hop) % members), owner),
            device_id_type=MESH,
        )

    def share_gains(hop):
        target = ring_member((place + hop) % members)
        return pltpu.make_async_remote_copy(
            src_ref=gains_ref.at[target * sub // UNIT],
            dst_ref=final_ref.at[members - hop],
            send_sem=g_send.at[hop - 1],
            recv_sem=g_recv.at[hop - 1],
            device_id=(target, owner),
            device_id_type=MESH,
        )

    def prepare(f):
        fetch(f).wait()
        block = jnp.dot(
            table_ref[...],
            sketch_part_ref[f],
            preferred_element_type=jnp.float32,
        ).astype(out_ref.dtype)
        out_ref[f] = block.reshape(out_ref.shape[1:])
        rows_ref[0, f, :, owner] = out_ref[f, owner]

    def part_rows(slot, f):
        return rows_ref[slot, f].reshape(capacity, part)

    def multiply(slot, f, left=0, first=0, last=chunks):
        low, high = first * lanes, last * lanes
        block = rows_ref[slot, f, first:last].reshape(high - low, part)
        product = dot_rows(part_rows(left, f), block)
        for chunk in range(first, last):
            cut = slice(chunk * lanes - low, (chunk + 1) * lanes - low)
            inner_ref[slot * chunks + chunk] += product[:, cut]
        total = jnp.zeros((high - low, 128), jnp.float32)
        for spot in range(0, part, 128):
            wide = block[:, spot : spot + 128].astype(jnp.float32)
            total = total + wide * wide
        squares_ref[slot, low:high] += total

    def multiply_picks(slot, f, picks, first=0, last=chunks):
        low, high = first * lanes, last * lanes
        block = rows_ref[slot, f, first:last].reshape(high - low, part)
        pick_inner_ref[slot, :, low:high] += dot_rows(picks, block)

    def own_part(f):
        picks_ref[0, f] = lax.dot_general(
            pick_table,
            part_rows(0, f),
            (((1,), (0,)), ((), ())),
            preferred_element_type=jnp.float32,
        ).astype(picks_ref.dtype)
        multiply(0, f)
        for hop in range(1, members):
            share_picks(f, hop).start()

    def other_part(f, forward=True):
        for pair in range(pairs):
            for hop in range(1, half):
                share(f, hop, pair).wait_recv()

            if forward:

                @pl.when(gives_first)
                def _(pair=pair):
                    share_first(f, pair).start()

        for hop in range(1, members):
            share_picks(f, hop).wait_recv()
        picks = picks_ref[0, f].astype(jnp.float32)
        for hop in range(1, members):
            picks = picks + picks_ref[hop, f].astype(jnp.float32)
        total = jnp.zeros((PICK_ROWS, 128), jnp.float32)
        for low in range(0, part, 128):
            wide = picks[:, low : low + 128]
            total = total + wide * wide
        pick_squares_ref[...] += total
        picks = picks.astype(picks_ref.dtype)
        multiply_picks(0, f, picks)
        for hop in range(1, half):
            multiply(hop, f)
            multiply_picks(hop, f, picks)

        @pl.when(gets_second)
        def _():
            for pair in range(pairs):
                share_second(f, pair).wait_recv()
            multiply(half, f, 1, cut_chunk, chunks)
            multiply_picks(half, f, picks, cut_chunk, chunks)

        @pl.when(gets_first)
        def _():
            for pair in range(pairs):
                share_first(f, pair).wait_recv()
            multiply(half, f, 0, 0, cut_chunk)
            multiply_picks(half, f, picks, 0, cut_chunk)

    for f in range(parts):
        fetch(f).start()
    label_bits, place_bits, sub_bits = bits(members), bits(members * owners * sub), bits(sub)
    unit_bits = bits(UNIT)
    places = places_ref[...]
    target = (labels_ref[...] << label_bits) + (places >> place_bits)
    target = (target << sub_bits) + (places & (sub - 1))
    table_ref[...] = (
        lax.broadcasted_iota(jnp.int32, (2 * row_count, row_count), 0) == target
    ).astype(table_ref.dtype)
    for f in range(window + 1):
        prepare(f)
    pl.semaphore_wait(barrier, owners + members - 2)
    for f in range(window):
        dispatch_all(f)

    inner_ref[...] = jnp.zeros_like(inner_ref)
    pick_inner_ref[...] = jnp.zeros_like(pick_inner_ref)
    squares_ref[...] = jnp.zeros_like(squares_ref)
    pick_squares_ref[...] = jnp.zeros_like(pick_squares_ref)
    row_gain_ref[...] = jnp.zeros_like(row_gain_ref)

    chosen = pick_ref[...]
    source = (chosen & (members * owners * sub - 1)) >> sub_bits
    offset = ((chosen >> place_bits) << sub_bits) + (chosen & (sub - 1))
    chosen = ((offset >> unit_bits) << bits(owners)) + (source & (owners - 1))
    chosen = (chosen << unit_bits) + (offset & (UNIT - 1)) + (source >> bits(owners)) * capacity
    turn_row = lax.broadcasted_iota(jnp.int32, (PICK_ROWS, capacity), 0)
    wanted = jnp.full((PICK_ROWS, capacity), -1, jnp.int32)
    for turn in range(steps):
        wanted = jnp.where(turn_row == turn, chosen[:, turn : turn + 1], wanted)
    pick_table = (
        lax.broadcasted_iota(jnp.int32, (PICK_ROWS, capacity), 1) + member * capacity == wanted
    ).astype(rows_ref.dtype)

    lows = UNIT // sub
    lane = lax.broadcasted_iota(jnp.int32, (members * owners, lanes), 1)
    source = lax.broadcasted_iota(jnp.int32, (members * owners, lanes), 0)
    spot = lax.broadcasted_iota(jnp.int32, (1, lanes), 1) & (sub - 1)
    for ahead in range(members):
        block = ring_member((place + ahead) % members)
        filled = jnp.zeros((chunks, lanes), jnp.float32)
        for low in range(lows):
            spread_out = (source == block * owners + (lane >> unit_bits)) & (
                ((lane >> sub_bits) & (lows - 1)) == low
            )
            filled = filled + jnp.dot(
                counts_ref[low].astype(jnp.float32).astype(jnp.bfloat16),
                spread_out.astype(jnp.bfloat16),
                preferred_element_type=jnp.float32,
            )
        place_ref[ahead] = (filled > spot.astype(jnp.float32)).astype(jnp.float32)
    total = jnp.sum(counts_ref[...].astype(jnp.float32), axis=0)
    total = jnp.sum(jnp.sum(total, axis=0, keepdims=True), axis=1, keepdims=True)

    @pl.loop(0, parts)
    def _(f):
        for pair in range(pairs):
            for mask in (2 * pair, 2 * pair + 1):
                if mask:
                    dispatch(f, mask).wait_recv()
            for hop in range(1, half):
                share(f, hop, pair).start()

            @pl.when(gives_second)
            def _(pair=pair):
                share_second(f, pair).start()

            @pl.when(gives_second & (f == parts - 1))
            def _(pair=pair):
                share_direct(f, pair).start()

        @pl.when(f + window < parts)
        def _():
            dispatch_all(f + window)

        @pl.when(f + window + 1 < parts)
        def _():
            prepare(f + window + 1)

        own_part(f)

        @pl.when(f > 0)
        def _():
            other_part(f - 1)

    other_part(parts - 1, forward=False)

    def block_row(behind):
        rows = place_ref[(members * half - step * behind) % members]
        return jnp.concatenate([rows[chunk : chunk + 1] for chunk in range(chunks)], axis=1)

    def valid_row(slot):
        if slot < half:
            return block_row(slot)
        split = cut_chunk * lanes
        first = jnp.where(gets_first, block_row(half)[:, :split], 0.0)
        second = jnp.where(gets_second, block_row(half + 1)[:, split:], 0.0)
        return jnp.concatenate([first, second], axis=1)

    def turned(row):
        return jnp.transpose(jnp.broadcast_to(row, (128, capacity)))

    valid = [valid_row(slot) > 0.5 for slot in range(slots)]
    norm = [
        jnp.sum(jnp.transpose(squares_ref[slot]), axis=0, keepdims=True) * scale
        for slot in range(slots)
    ]
    pick_norm = jnp.sum(pick_squares_ref[...], axis=1, keepdims=True) * scale

    def repeat(block):
        if lanes > 128:
            block = jnp.concatenate([block] * (lanes // 128), axis=1)
        return block

    def left_of(slot, chunk):
        return 1 if slot == half and chunk >= cut_chunk else 0

    tops = []
    for slot in range(slots):
        held = []
        for turn in range(steps):
            apart = (
                pick_norm[turn : turn + 1]
                + norm[slot]
                - (2.0 * scale) * pick_inner_ref[slot][turn : turn + 1]
            )
            held.append(jnp.minimum(held[-1], apart) if held else apart)
        tops.append(held)

    for left in range(2):
        closed = turned(jnp.where(valid[left], -norm[left], -FAR))
        wide_ref[left, steps] = closed
        wide_ref[left, 0] = jnp.where(closed > -0.5 * FAR, -closed, -FAR)
        for turn in range(1, steps):
            wide_ref[left, turn] = turned(
                jnp.where(valid[left], tops[left][turn - 1] - norm[left], -FAR)
            )

    largest = jnp.zeros((1, lanes), jnp.float32)
    for slot in range(slots):
        for chunk in range(chunks):
            cut = slice(chunk * lanes, (chunk + 1) * lanes)
            near = repeat(wide_ref[left_of(slot, chunk), 0])
            there = jnp.where(valid[slot][:, cut], norm[slot][:, cut], FAR)
            tile = (2.0 * scale) * inner_ref[slot * chunks + chunk] - there
            inner_ref[slot * chunks + chunk] = tile
            tile = jnp.max(near - tile, axis=0, keepdims=True)
            largest = jnp.maximum(largest, jnp.where(valid[slot][:, cut], tile, 0.0))
    largest = jnp.max(largest, axis=1, keepdims=True)
    bound_ref[0] = jnp.broadcast_to(largest, bound_ref.shape[1:])
    for hop in range(1, members):
        share_bound(hop).start()
    for left in range(2):
        wide_ref[left, 0] = wide_ref[left, steps] + largest

    sizes = [
        jnp.sum(valid[left].astype(jnp.float32), axis=1, keepdims=True) for left in range(2)
    ]
    far_sizes = [jnp.zeros((1, 1), jnp.float32) for left in range(2)]

    for slot in range(slots):
        for chunk in range(chunks):
            cut = slice(chunk * lanes, (chunk + 1) * lanes)
            tile = inner_ref[slot * chunks + chunk]
            gained = []
            left = left_of(slot, chunk)
            if slot > 0:
                closed = tile + repeat(wide_ref[left, steps])
            for turn in range(steps):
                each = jnp.maximum(tile + repeat(wide_ref[left, turn]), 0.0)
                gained.append(jnp.sum(each, axis=0, keepdims=True))
                if slot > 0:
                    if turn > 0:
                        each = jnp.maximum(closed + tops[slot][turn - 1][:, cut], 0.0)
                    for low in range(0, lanes, 128):
                        row_gain_ref[left, turn] += each[:, low : low + 128]
            gained.append(
                tops[0][steps - 1][:, cut] if slot == 0 else jnp.zeros((1, lanes), jnp.float32)
            )
            gained.append(jnp.broadcast_to(largest * sizes[left], (1, lanes)))
            if slot == half:
                gets = gets_second if left else gets_first
                gained = [jnp.where(gets, row, 0.0) for row in gained]
            if slot > 0:
                far_sizes[left] = far_sizes[left] + jnp.sum(
                    valid[slot][:, cut].astype(jnp.float32), axis=1, keepdims=True
                )
            gained.append(jnp.zeros((8 - steps - 2, lanes), jnp.float32))
            gains_ref[chunk, slot] = jnp.concatenate(gained, axis=0)
    for left in range(2):
        for turn in range(steps):
            row = jnp.sum(jnp.transpose(row_gain_ref[left, turn]), axis=0, keepdims=True)
            for chunk in range(chunks):
                cut = slice(chunk * lanes, (chunk + 1) * lanes)
                gains_ref[chunk, left, turn : turn + 1] += row[:, cut]
        for chunk in range(chunks):
            gains_ref[chunk, left, steps + 1 : steps + 2] += jnp.broadcast_to(
                largest * far_sizes[left], (1, lanes)
            )

    for hop in range(1, members):
        share_gains(hop).start()
    final_ref[0] = gains_ref[member * sub // UNIT]

    @pl.loop(0, parts)
    def _(f):
        for mask in range(1, owners):
            dispatch(f, mask).wait_send()
        for pair in range(pairs):
            for hop in range(1, half):
                share(f, hop, pair).wait_send()
        for hop in range(1, members):
            share_picks(f, hop).wait_send()

        @pl.when(gives_second)
        def _():
            for pair in range(pairs):
                share_second(f, pair).wait_send()

        @pl.when(gives_second & (f == parts - 1))
        def _():
            for pair in range(pairs):
                share_direct(f, pair).wait_send()

        @pl.when(gives_first & (f < parts - 1))
        def _():
            for pair in range(pairs):
                share_first(f, pair).wait_send()

    for hop in range(1, members):
        share_bound(hop).wait_recv()
    bound = bound_ref[0]
    for hop in range(1, members):
        bound = jnp.maximum(bound, bound_ref[hop])
    bound = bound[:1, :1]
    for hop in range(1, members):
        share_gains(hop).wait_recv()
    chunk_here = member * sub // UNIT
    second = chunk_here // cut_chunk
    for ahead in range(members):
        summed = final_ref[ahead, 0]
        for slot in range(1, slots):
            behind = slot if slot < half else half + second
            holder = (ahead + step * behind + members * half) % members
            summed = summed + final_ref[holder, slot]
        block = ring_member((place + ahead) % members)
        here = pl.ds(pl.multiple_of(block * lanes, lanes), lanes)
        used = place_ref[ahead, pl.ds(chunk_here, 1)]
        for turn in range(steps):
            row = summed[turn : turn + 1]
            if turn == 0:
                row = row + (total * bound - summed[steps + 1 : steps + 2])
            gain_ref[turn, :, here] = row * used / total
        cover_ref[:, here] = jnp.maximum(bound - summed[steps : steps + 1], 0.0) * used

    for hop in range(1, members):
        share_bound(hop).wait_send()
        share_gains(hop).wait_send()


def class_gains(labels, places, picks, counts, sketches, members, owners, sub, steps):
    row_count, width = sketches.shape
    chunks = members * sub // UNIT
    lanes = owners * UNIT
    capacity = chunks * lanes
    slots = members // 2 + 1
    part = width // PARTS
    kind = sketches.dtype
    vmem = pl.BlockSpec(memory_space=pltpu.VMEM)
    dma = pltpu.SemaphoreType.DMA
    return pl.pallas_call(
        functools.partial(class_kernel, members, owners, sub, steps),
        out_shape=(
            jax.ShapeDtypeStruct((steps, 1, members * lanes), jnp.float32),
            jax.ShapeDtypeStruct((1, members * lanes), jnp.float32),
        ),
        in_specs=[vmem, vmem, vmem, vmem, pl.BlockSpec(memory_space=pl.ANY)],
        out_specs=(vmem, vmem),
        scratch_shapes=[
            pltpu.VMEM((PARTS, row_count, part), kind),
            pltpu.VMEM((2 * row_count, row_count), kind),
            pltpu.VMEM((PARTS, owners, chunks, UNIT, part), kind),
            pltpu.VMEM((slots, PARTS, chunks, owners, UNIT, part), kind),
            pltpu.VMEM((members, PARTS, PICK_ROWS, part), kind),
            pltpu.VMEM((members, chunks, lanes), jnp.float32),
            pltpu.VMEM((slots * chunks, capacity, lanes), jnp.float32),
            pltpu.VMEM((slots, PICK_ROWS, capacity), jnp.float32),
            pltpu.VMEM((slots, capacity, 128), jnp.float32),
            pltpu.VMEM((PICK_ROWS, 128), jnp.float32),
            pltpu.VMEM((members, 8, 128), jnp.float32),
            pltpu.VMEM((2, steps + 1, capacity, 128), jnp.float32),
            pltpu.VMEM((2, steps, capacity, 128), jnp.float32),
            pltpu.VMEM((chunks, slots, 8, lanes), jnp.float32),
            pltpu.VMEM((members, slots, 8, lanes), jnp.float32),
            dma((PARTS,)),
            dma((PARTS, owners - 1)),
            dma((PARTS, owners - 1)),
            dma((PARTS, members // 2 - 1, owners // 2)),
            dma((PARTS, members // 2 - 1, owners // 2)),
            dma((PARTS, 2, owners // 2)),
            dma((PARTS, 2, owners // 2)),
            dma((PARTS, members - 1)),
            dma((PARTS, members - 1)),
            dma((members - 1,)),
            dma((members - 1,)),
            dma((members - 1,)),
            dma((members - 1,)),
        ],
        compiler_params=pltpu.CompilerParams(
            collective_id=0, has_side_effects=True, vmem_limit_bytes=53 * 1024 * 1024
        ),
    )(labels, places, picks, counts, sketches)


def body(sketches, labels, places, counts, chosen):
    row_count = sketches.shape[0]
    members = lax.axis_size("dp")
    owners = lax.axis_size("cls")
    devices = members * owners
    sub = 2 * row_count // devices
    capacity = devices * sub
    chunks = members * sub // UNIT
    lows = UNIT // sub
    member = lax.axis_index("dp")
    steps = chosen.shape[0]

    filled = jnp.transpose(counts[0].reshape(chunks, lows, devices), (1, 0, 2))
    gain_scores, coverage = class_gains(
        labels.reshape(1, row_count),
        places.reshape(1, row_count),
        chosen.reshape(1, steps),
        filled,
        sketches,
        members,
        owners,
        sub,
        steps,
    )
    if lows > 1:
        gain_scores = lax.dynamic_index_in_dim(
            gain_scores.reshape(steps, 1, members * owners, lows, sub), member % lows, 3, False
        ).reshape(steps, 1, capacity)
        coverage = lax.dynamic_index_in_dim(
            coverage.reshape(1, members * owners, lows, sub), member % lows, 2, False
        ).reshape(1, capacity)
    return (gain_scores, coverage)


def solution(mesh):
    placed = (
        P(("dp", "cls"), None),
        P(("dp", "cls")),
        P(("dp", "cls")),
        P("cls", None, None),
        P(None, "cls"),
    )
    return jax.shard_map(
        body,
        mesh=mesh,
        in_specs=placed,
        out_specs=(P(None, "cls", "dp"), P("cls", "dp")),
        check_vma=False,
    )
```
